32 devices in a mesh: row: 4 (over x, core), col: 8 (over z, y).
Axes of the slice: x: 2, y: 2, z: 4, core: 2. Of those that a mesh axis runs over, the one named last changes fastest.
Arguments:
- ancestor_inv: bfloat16 [32, 32, 256, 256], P('row', 'col'), may hold values from -0.29882812 to 0.29882812
- lower_panel: bfloat16 [8, 16, 256, 256], P('row', 'col'), may hold values from -0.59765625 to 0.59765625
- upper_panel: bfloat16 [8, 16, 256, 256], P('col', 'row'), may hold values from -0.59765625 to 0.59765625
- pivot_inv: float32 [8, 256, 256], P('col'), may hold values from -6 to 6
- members: int32 [8, 16], replicated, may hold values from -1 to 31, as said below
Outputs:
- lower_inv: bfloat16 [8, 16, 256, 256], P('col', 'row')
- upper_inv: bfloat16 [8, 16, 256, 256], P('row', 'col')
- diag_inv: float32 [8, 256, 256], P('col')
The draws below stay inside these ranges and needn't reach their ends.
Inputs may be any that keep to these rules, and one draw needn't show every extreme that they name: `members`: slot s belongs to group g = s // 2; a used slot names an ancestor block of that group, from g * 4 to (g + 1) * 4 - 1. In each group of each supernode the used slots come first, name distinct blocks, and number 1 to 2; every group has 2 used slots for some supernode. Empty slots hold -1.
All inputs are finite; a program needn't handle non-finite values.
Results may differ from the reference program's by a relative error of at most 0.013.
Values may be sent and summed in bfloat16 or wider, within the bound.
A program may use at most 128 MiB of HBM per device.

```python
from functools import partial
import jax
import jax.numpy as jnp
from jax import lax

B = 256
NBC = 4
CAP = 2
KL = 8
NB = 32
SLOTS = 16


def draw_members(key, part):
    groups = SLOTS // CAP
    key_counts, key_fullrow, key_ranking = jax.random.split(key, 3)
    counts = jax.random.randint(key_counts, (KL, groups), 1, CAP + 1)
    full_row = jax.random.randint(key_fullrow, (groups,), 0, KL)
    counts = jnp.where(jnp.arange(KL)[:, None] == full_row[None, :], CAP, counts)
    scores = jax.random.randint(key_ranking, (KL, groups, NBC), 0, 1 << 20) * NBC + jnp.arange(NBC)[None, None, :]
    ranking = jnp.argsort(scores, axis=-1)[:, :, :CAP]
    blocks = ranking + (jnp.arange(groups) * NBC)[None, :, None]
    in_use = jnp.arange(CAP)[None, None, :] < counts[:, :, None]
    return jnp.where(in_use, blocks, -1).astype(jnp.int32).reshape(KL, SLOTS)


def steps_of(own_key, dims, pieces, least, largest):
    loudness = 1.0
    for dim, parts in pieces:
        heights = jax.random.uniform(jax.random.fold_in(jax.random.fold_in(own_key, 6), dim), (parts,), jnp.float32, least / len(pieces), largest / len(pieces))
        loudness = loudness * jnp.repeat(jnp.exp(heights), dims[dim] // parts).reshape((-1,) + (1,) * (len(dims) - 1 - dim))
    return loudness


def gaussian(stream_key, shape, spread, reach, shards=(), dtype=jnp.bfloat16):
    entries = spread * jax.random.normal(stream_key, shape, jnp.float32)
    if shards:
        entries = entries * steps_of(stream_key, shape, shards, -0.22, 0.18)
    return jnp.clip(entries, -reach, reach).astype(dtype)


def setup_inputs(seed: int = 0) -> dict:
    streams_of = jax.random.split(jax.random.key(seed), 6)
    return {
        "ancestor_inv": gaussian(streams_of[0], (NB, NB, B, B), 0.05, 0.29882812, ((0, 4), (1, 8))),
        "lower_panel": gaussian(streams_of[1], (KL, SLOTS, B, B), 0.1, 0.59765625, ((0, 4), (1, 8))),
        "upper_panel": gaussian(streams_of[2], (KL, SLOTS, B, B), 0.1, 0.59765625, ((0, 8), (1, 4))),
        "pivot_inv": gaussian(streams_of[3], (KL, B, B), 1.0, 6.0, ((0, 8),), jnp.float32),
        "members": draw_members(jax.random.fold_in(streams_of[5], 71), 0),
    }


def one_supernode(ancestor_inv, item):
    member_row, lower_blocks, upper_blocks, pivot_block = item
    valid = member_row >= 0
    chosen = jnp.where(valid, member_row, 0).astype(jnp.int32)
    strip = jnp.take(ancestor_inv, chosen, axis=0)
    square = jnp.take(strip, chosen, axis=1).astype(jnp.float32)
    weight = valid.astype(jnp.float32)[:, None, None]
    lower_masked = lower_blocks.astype(jnp.float32) * weight
    upper_masked = upper_blocks.astype(jnp.float32) * weight
    lower_sum = -jnp.einsum("ijab,jbc->iac", square, lower_masked) * weight
    lower_inv = lower_sum.astype(jnp.bfloat16)
    upper_sum = -jnp.einsum("iab,ijbc->jac", upper_masked, square) * weight
    upper_inv = upper_sum.astype(jnp.bfloat16)
    diag_inv = pivot_block - jnp.einsum("iab,ibc->ac", upper_masked, lower_inv.astype(jnp.float32))
    return lower_inv, upper_inv, diag_inv


def reference(ancestor_inv, lower_panel, upper_panel, pivot_inv, members):
    lower_inv, upper_inv, diag_inv = lax.map(partial(one_supernode, ancestor_inv), (members, lower_panel, upper_panel, pivot_inv))
    return (lower_inv, upper_inv, diag_inv)
```

```python
import functools

import jax
import jax.numpy as jnp
from jax import lax
from jax.experimental import pallas as pl
from jax.experimental.pallas import tpu as pltpu
from jax.sharding import PartitionSpec as P

NY = 2
CORES = 2
BF = jnp.bfloat16
F32 = jnp.float32


def kernel(
    n_row, n_col, nq, nf,
    mem_in, anc, low, upp, piv_in,
    low_out, upp_out, diag_out,
    mem, piv, a, lbuf, ubuf, pl_buf, yr, zr, zq, pu, pr, ur, ds, dr, acc, dacc,
    loc, l_s, l_rel, l_r, uy_s, uy_r, uz_s, uz_r, ry_s, ry_r, rz_s, rz_r, rq_s, rq_r,
    pr_s, pr_r, pu_s, pu_r, d_s, d_r,
):
    row = lax.axis_index("row")
    col = lax.axis_index("col")
    nz = n_col // NY
    nx = n_row // CORES
    x, core = row // CORES, row % CORES
    z, y = col // NY, col % NY
    yp = z * NY + (1 - y)
    rb, cb = anc.shape[0], anc.shape[1]
    kr, cs = low.shape[0], low.shape[1]
    rs = upp.shape[1]
    ny_blocks = rs - nq
    nyf = rs - nf
    partner = x * CORES + (1 - core)

    def remote(src, dst, ss, rsem, **where):
        return pltpu.make_async_remote_copy(
            src_ref=src, dst_ref=dst, send_sem=ss, recv_sem=rsem, device_id=where
        )

    ca = pltpu.make_async_copy(anc, a, loc.at[0])
    cl = pltpu.make_async_copy(low, lbuf.at[pl.ds(row * kr, kr)], loc.at[1])
    cu = pltpu.make_async_copy(upp.at[0], ubuf.at[col], loc.at[2])
    cp = pltpu.make_async_copy(piv_in.at[0], piv, loc.at[3])
    cm = pltpu.make_async_copy(mem_in, mem, loc.at[4])
    cm.start()
    cl.start()
    cu.start()
    ca.start()
    cp.start()

    bar = pltpu.get_barrier_semaphore()
    for dx in range(1, n_row):
        pl.semaphore_signal(bar, inc=1, device_id={"row": (row + dx) % n_row})
    pl.semaphore_signal(bar, inc=1, device_id={"col": yp})

    @pl.when(z > 0)
    def _():
        pl.semaphore_signal(bar, inc=1, device_id={"col": col - NY})

    @pl.when(z < nz - 1)
    def _():
        pl.semaphore_signal(bar, inc=1, device_id={"col": col + NY})

    peers = n_row + jnp.where(z > 0, 1, 0) + jnp.where(z < nz - 1, 1, 0)
    pl.semaphore_wait(bar, peers)

    def l_own(r2):
        return remote(low, lbuf.at[pl.ds(row * kr, kr)], l_s.at[r2], l_r.at[row], row=r2)

    def l_recv(r2):
        blk = lbuf.at[pl.ds(r2 * kr, kr)]
        return remote(blk, blk, l_rel.at[r2], l_r.at[r2], row=partner)

    def uy_own(kind):
        part = pl.ds(0, ny_blocks) if kind else pl.ds(ny_blocks, nq)
        return remote(
            upp.at[0, part], ubuf.at[col, part], uy_s.at[nz if kind == 0 else z],
            uy_r.at[nz if kind == 0 else z], col=yp,
        )

    def uy_got(kind, zs):
        part = pl.ds(0, ny_blocks) if kind else pl.ds(ny_blocks, nq)
        blk = ubuf.at[zs * NY + (1 - y), part]
        return remote(blk, blk, uy_s.at[zs], uy_r.at[nz if kind == 0 else zs], col=yp)

    def uy_pass(zs):
        blk = ubuf.at[zs * NY + y, pl.ds(0, ny_blocks)]
        return remote(blk, blk, uy_s.at[zs], uy_r.at[zs], col=yp)

    def uz(zs, kind, up):
        if kind == 0:
            blk = ubuf.at[zs * NY + y]
        else:
            blk = ubuf.at[zs * NY + (1 - y), pl.ds(ny_blocks, nq)]
        to = col + NY if up else col - NY
        return remote(blk, blk, uz_s.at[zs, int(up), kind], uz_r.at[zs, kind], col=to)

    def uz_own(up):
        to = col + NY if up else col - NY
        return remote(upp.at[0], ubuf.at[col], uz_s.at[z, int(up), 0], uz_r.at[z, 0], col=to)

    def ry(zd, h):
        return remote(
            pl_buf.at[zd * NY + (1 - y), h], yr.at[zd, h], ry_s.at[zd, h], ry_r.at[zd, h], col=yp
        )

    def rz(zd, h, up):
        slot = zd + 1 if up else zd
        to = col + NY if up else col - NY
        return remote(
            pl_buf.at[zd * NY + y, h], zr.at[slot, h], rz_s.at[zd, h], rz_r.at[slot, h], col=to
        )

    def rq(zd, f, up):
        slot = zd + 1 if up else zd
        to = col + NY if up else col - NY
        return remote(
            pl_buf.at[zd * NY + (1 - y), nyf + f], zq.at[slot, f], rq_s.at[zd, f],
            rq_r.at[slot, f], col=to,
        )

    def pr_copy(k):
        return remote(pu.at[k], pr.at[k], pr_s.at[k], pr_r.at[k], row=partner)

    def pu_copy(k):
        return remote(pu.at[k], ur.at[x, k % kr], pu_s.at[k], pu_r.at[x, k % kr], row=k // kr)

    def pu_got(x2, p):
        return remote(
            pu.at[0], ur.at[x2, p], pu_s.at[0], pu_r.at[x2, p], row=x2 * CORES + core
        )

    def keeps(k):
        return (k // kr) % CORES == core

    def leaves(k):
        return k // (kr * CORES) != x

    def d_copy(r2):
        return remote(ds, dr.at[row], d_s.at[r2], d_r.at[row], row=r2)

    def d_got(r2):
        return remote(ds, dr.at[r2], d_s.at[r2], d_r.at[r2], row=r2)

    def d_relay(x2):
        r2 = x2 * CORES + core
        blk = dr.at[r2]
        return remote(blk, blk, d_s.at[x2 * CORES + 1 - core], d_r.at[r2], row=partner)

    def each_dir(fn):
        @pl.when(z > 0)
        def _():
            fn(False)

        @pl.when(z < nz - 1)
        def _():
            fn(True)

    def row_member(k, i):
        m = mem[k, row * rs + i]
        return m >= 0, jnp.clip(m - row * rb, 0, rb - 1)

    def col_member(k, j):
        m = mem[k, col * cs + j]
        return m >= 0, jnp.clip(m - col * cb, 0, cb - 1)

    zero = jnp.zeros((), BF)

    def lower_part(k):
        cols = [col_member(k, j) for j in range(cs)]
        panels = [jnp.where(cols[j][0], lbuf[k, j], zero) for j in range(cs)]

        def one(i, _):
            ok, ri = row_member(k, i)
            tot = None
            for j in range(cs):
                t = jnp.dot(a[ri, cols[j][1]], panels[j], preferred_element_type=F32)
                tot = t if tot is None else tot + t
            pl_buf[k, i] = jnp.where(ok, tot, 0.0).astype(BF)
            return 0

        lax.fori_loop(0, rs, one, 0)

    def upper_part(k):
        rows = [row_member(k, i) for i in range(rs)]

        def one(j, _):
            ok, cj = col_member(k, j)
            tot = None
            for i in range(rs):
                t = jnp.dot(
                    jnp.where(rows[i][0], ubuf[k, i], zero), a[rows[i][1], cj],
                    preferred_element_type=F32,
                )
                tot = t if tot is None else tot + t
            pu[k, j] = jnp.where(ok, tot, 0.0).astype(BF)
            return 0

        lax.fori_loop(0, cs, one, 0)

        @pl.when(jnp.logical_not(keeps(k)))
        def _():
            pr_copy(k).start()

    def finish(k):
        @pl.when(jnp.logical_and(keeps(k), leaves(k)))
        def _():
            pr_copy(k).wait_recv()
            for j in range(cs):
                pu[k, j] = (pu[k, j].astype(F32) + pr[k, j].astype(F32)).astype(BF)
            pu_copy(k).start()

    def lower_group(r2):
        def one(p, _):
            k = r2 * kr + (p + 1 - y) % NY
            lower_part(k)

            @pl.when(k % NY != y)
            def _():
                for h in range(nyf):
                    ry(k // NY, h).start()

            return 0

        lax.fori_loop(0, kr, one, 0)

    def target(t):
        x2 = (x + t // CORES) % nx
        q = t % CORES
        return x2 * CORES + jnp.where(2 * x2 >= nx, CORES - 1 - q, q)

    def both_groups(x2):
        def one(q, _):
            lower_group(x2 * CORES + jnp.where(2 * x2 >= nx, CORES - 1 - q, q))
            return 0

        lax.fori_loop(0, CORES, one, 0)

    l_own(partner).start()
    for dx in range(1, nx):
        l_own(((x + dx) % nx) * CORES + core).start()
    uy_own(0).start()
    each_dir(lambda up: uz_own(up).start())

    cm.wait()
    ca.wait()
    cl.wait()
    l_recv(partner).wait_recv()
    both_groups(x)

    uy_got(0, z).wait_recv()
    each_dir(lambda up: uz(z, 1, up).start())
    cu.wait()
    upper_part(col)

    def others(fn):
        for dx in range(1, nx):
            fn((x + dx) % nx)

    def relay(x2):
        l_recv(x2 * CORES + core).wait_recv()
        l_recv(x2 * CORES + core).start()

    others(relay)

    def by_side(d, fn):
        @pl.when(z - d >= 0)
        def _():
            fn(z - d, True)

        @pl.when(z + d <= nz - 1)
        def _():
            fn(z + d, False)

    def take(kind):
        def one(zs, up):
            uz(zs, kind, up).wait_recv()

            @pl.when((z < nz - 1) if up else (z > 0))
            def _():
                uz(zs, kind, up).start()

        return one

    by_side(1, take(0))

    def late(x2):
        l_recv(x2 * CORES + 1 - core).wait_recv()
        both_groups(x2)

    others(late)
    uy_own(1).start()
    by_side(1, lambda zs, up: uy_pass(zs).start())
    by_side(1, take(1))

    def sides(d, fn):
        def one(s, _):
            zs = z + (2 * s - 1) * d

            @pl.when(jnp.logical_and(zs >= 0, zs < nz))
            def _():
                fn(zs)

            return 0

        lax.fori_loop(0, 2, one, 0)

    def near(d):
        sides(d, lambda zs: upper_part(zs * NY + y))

    def near_done(d):
        sides(d, lambda zs: finish(zs * NY + y))

    def far(d):
        def one(zs):
            uy_got(1, zs).wait_recv()
            upper_part(zs * NY + (1 - y))

        sides(d, one)

    def far_done(d):
        sides(d, lambda zs: finish(zs * NY + (1 - y)))

    def add_to(k, h, terms):
        tot = pl_buf[k, h].astype(F32)
        for t in terms:
            tot = tot + t.astype(F32)
        pl_buf[k, h] = tot.astype(BF)

    def hop(zd, h, own, waits_y):
        k = zd * NY + (y if own else 1 - y)

        def go(up):
            slot = zd + 1 if up else zd
            step = rz(zd, h, up) if own else rq(zd, h - nyf, up)
            if waits_y:
                ry(zd, h).wait_recv()

            @pl.when((z > 0) if up else (z < nz - 1))
            def _():
                step.wait_recv()
                part = zr[slot, h] if own else zq[slot, h - nyf]
                add_to(k, h, [yr[zd, h], part] if waits_y else [part])

            if waits_y:
                @pl.when((z == 0) if up else (z == nz - 1))
                def _():
                    add_to(k, h, [yr[zd, h]])

            step.start()

        @pl.when(zd > z)
        def _():
            go(True)

        @pl.when(zd < z)
        def _():
            go(False)

    def bands(zds):
        for f in range(nyf, rs):
            for zd, ok in zds:
                @pl.when(ok)
                def _():
                    hop(zd, f, True, False)
                    hop(zd, f, False, False)

        def piece(h, _):
            for zd, ok in zds:
                @pl.when(ok)
                def _():
                    hop(zd, h, True, True)

            return 0

        lax.fori_loop(0, nyf, piece, 0)

    def chain(t):
        zd = target(t)
        bands([(zd, zd != z)])

    near(1)
    finish(col)
    edge = jnp.logical_or(z == 0, z == nz - 1)

    def take_pass(d):
        by_side(d, take(0))
        by_side(d, lambda zs, up: uy_pass(zs).start())
        by_side(d, take(1))
        near(d)
        near_done(d - 1)

    @pl.when(edge)
    def _():
        def first(t, _):
            chain(t)
            return 0

        lax.fori_loop(0, CORES, first, 0)

        def one(d, _):
            chain(CORES + d - 2)
            take_pass(d)
            return 0

        lax.fori_loop(2, nz, one, 0)
        near_done(nz - 1)

    @pl.when(jnp.logical_not(edge))
    def _():
        def one(d, _):
            take_pass(d)
            return 0

        lax.fori_loop(2, nz - 1, one, 0)
        near_done(nz - 2)
        low_half = 2 * z < nz
        short = jnp.where(low_half, z, nz - 1 - z)
        gap = nz - 1 - 2 * short

        def pair(s, _):
            s2 = s - gap
            bands([
                (jnp.where(low_half, nz - 1 - s, s), s >= 0),
                (jnp.where(low_half, s2, nz - 1 - s2), s2 >= 0),
            ])
            return 0

        lax.fori_loop(0, nz - 1 - short, pair, 0)

    for f in range(nf):
        k2 = z * NY + (1 - y)
        each_dir(lambda up: rq(z, f, not up).wait_recv())

        @pl.when(z > 0)
        def _():
            add_to(k2, nyf + f, [zq[z + 1, f]])

        @pl.when(z < nz - 1)
        def _():
            add_to(k2, nyf + f, [zq[z, f]])

        ry(z, nyf + f).start()

    uy_got(1, z).wait_recv()
    upper_part(yp)
    far(1)
    finish(yp)

    def final(h, _):
        ry(z, h).wait_recv()
        acc[h] = pl_buf[col, h].astype(F32) + yr[z, h].astype(F32)

        @pl.when(z > 0)
        def _():
            rz(z, h, True).wait_recv()
            acc[h] = acc[h] + zr[z + 1, h].astype(F32)

        @pl.when(z < nz - 1)
        def _():
            rz(z, h, False).wait_recv()
            acc[h] = acc[h] + zr[z, h].astype(F32)

        low_out[0, h] = (-acc[h]).astype(BF)
        return 0

    lax.fori_loop(0, rs, final, 0)
    tot = None
    for i in range(rs):
        t = jnp.dot(
            jnp.where(row_member(col, i)[0], ubuf[col, i], zero), low_out[0, i],
            preferred_element_type=F32,
        )
        tot = t if tot is None else tot + t
    dacc[...] = tot
    ds[...] = tot.astype(BF)
    others(lambda x2: d_copy(x2 * CORES + core).start())
    d_copy(partner).start()

    def far_rest(d, _):
        far(d)
        far_done(d - 1)
        return 0

    lax.fori_loop(2, nz, far_rest, 0)
    far_done(nz - 1)

    def d_pass(x2):
        d_got(x2 * CORES + core).wait_recv()
        d_relay(x2).start()

    def d_add(r2):
        dacc[...] = dacc[...] + dr[r2].astype(F32)

    others(d_pass)
    d_got(partner).wait_recv()
    d_add(partner)

    def d_add_chip(x2):
        d_add(x2 * CORES + core)
        d_got(x2 * CORES + 1 - core).wait_recv()
        d_add(x2 * CORES + 1 - core)

    others(d_add_chip)
    cp.wait()
    diag_out[0] = piv[...] - dacc[...]

    for p in range(kr):
        pr_copy(row * kr + p).wait_recv()
        for j in range(cs):
            acc[p * cs + j] = pu[row * kr + p, j].astype(F32) + pr[row * kr + p, j].astype(F32)

    def pu_add(x2):
        for p in range(kr):
            pu_got(x2, p).wait_recv()
            for j in range(cs):
                acc[p * cs + j] = acc[p * cs + j] + ur[x2, p, j].astype(F32)

    others(pu_add)
    for p in range(kr):
        for j in range(cs):
            upp_out[p, j] = (-acc[p * cs + j]).astype(BF)

    l_own(partner).wait_send()
    for dx in range(1, nx):
        r2 = ((x + dx) % nx) * CORES + core
        l_own(r2).wait_send()
        l_recv(r2).wait_send()
    uy_own(0).wait_send()
    uy_own(1).wait_send()

    def own_done(up):
        uz_own(up).wait_send()
        uz(z, 1, up).wait_send()

    each_dir(own_done)

    def passed(zs, up):
        uy_pass(zs).wait_send()

        @pl.when((z < nz - 1) if up else (z > 0))
        def _():
            for kind in range(2):
                uz(zs, kind, up).wait_send()

    for d in range(1, nz):
        by_side(d, passed)

    def sums_done(zd, _):
        for h in range(nyf):
            ry(zd, h).wait_send()

        def along(up):
            for h in range(rs):
                rz(zd, h, up).wait_send()
            for f in range(nf):
                rq(zd, f, up).wait_send()

        @pl.when(zd > z)
        def _():
            along(True)

        @pl.when(zd < z)
        def _():
            along(False)

        return 0

    lax.fori_loop(0, nz, sums_done, 0)
    for f in range(nf):
        ry(z, nyf + f).wait_send()

    def parts_done(k, _):
        @pl.when(jnp.logical_not(keeps(k)))
        def _():
            pr_copy(k).wait_send()

        @pl.when(jnp.logical_and(keeps(k), leaves(k)))
        def _():
            pu_copy(k).wait_send()

        return 0

    lax.fori_loop(0, n_col, parts_done, 0)
    d_copy(partner).wait_send()

    def d_done(x2):
        d_copy(x2 * CORES + core).wait_send()
        d_relay(x2).wait_send()

    others(d_done)


def hand_over(*refs):
    sems = refs[-1]
    copies = [
        pltpu.make_async_copy(src, dst, sems.at[i])
        for i, (src, dst) in enumerate(zip(refs[:3], refs[3:6]))
    ]
    for c in copies:
        c.start()
    for c in copies:
        c.wait()


def body(ancestor_inv, lower_panel, upper_panel, pivot_inv, members):
    n_col = lax.axis_size("col")
    n_row = lax.axis_size("row")
    side = ancestor_inv.shape[2]
    rb, cb = ancestor_inv.shape[:2]
    kr, cs = lower_panel.shape[:2]
    per_col, rs = upper_panel.shape[:2]
    level = members.shape[0]
    nz = n_col // NY
    assert per_col == 1 and level == n_col and kr == NY and nz == n_row
    nf = max(1, rs // 4)
    nq = rs // 2
    blk = (side, side)
    dma = pltpu.SemaphoreType.DMA
    vmem = pl.BlockSpec(memory_space=pltpu.VMEM)
    hbm = pl.BlockSpec(memory_space=pltpu.HBM)
    outs = pl.pallas_call(
        functools.partial(kernel, n_row, n_col, nq, nf),
        out_shape=(
            pltpu.VMEM((per_col, rs) + blk, BF),
            pltpu.VMEM((kr, cs) + blk, BF),
            pltpu.VMEM((per_col,) + blk, F32),
        ),
        in_specs=[hbm] * 5,
        out_specs=(vmem, vmem, vmem),
        scratch_shapes=[
            pltpu.SMEM(members.shape, jnp.int32),
            pltpu.VMEM(blk, F32),
            pltpu.VMEM((rb, cb) + blk, BF),
            pltpu.VMEM((level, cs) + blk, BF),
            pltpu.VMEM((n_col, rs) + blk, BF),
            pltpu.VMEM((n_col, rs) + blk, BF),
            pltpu.VMEM((nz, rs) + blk, BF),
            pltpu.VMEM((nz + 1, rs) + blk, BF),
            pltpu.VMEM((nz + 1, nf) + blk, BF),
            pltpu.VMEM((level, cs) + blk, BF),
            pltpu.VMEM((level, cs) + blk, BF),
            pltpu.VMEM((n_row // CORES, kr, cs) + blk, BF),
            pltpu.VMEM(blk, BF),
            pltpu.VMEM((n_row,) + blk, BF),
            pltpu.VMEM((max(rs, kr * cs),) + blk, F32),
            pltpu.VMEM(blk, F32),
            dma((5,)), dma((n_row,)), dma((n_row,)), dma((n_row,)),
            dma((nz + 1,)), dma((nz + 1,)), dma((nz, 2, 2)), dma((nz, 2)),
            dma((nz, rs)), dma((nz, rs)), dma((nz, rs)), dma((nz + 1, rs)),
            dma((nz, nf)), dma((nz + 1, nf)), dma((n_col,)), dma((n_col,)),
            dma((n_col,)), dma((n_row // CORES, kr)), dma((n_row,)), dma((n_row,)),
        ],
        compiler_params=pltpu.CompilerParams(
            collective_id=0, has_side_effects=True, vmem_limit_bytes=60 * 1024 * 1024
        ),
    )(members, ancestor_inv, lower_panel, upper_panel, pivot_inv)
    return pl.pallas_call(
        hand_over,
        out_shape=tuple(jax.ShapeDtypeStruct(o.shape, o.dtype) for o in outs),
        in_specs=[vmem] * 3,
        out_specs=(hbm,) * 3,
        scratch_shapes=[dma((3,))],
    )(*(pltpu.with_memory_space_constraint(o, pltpu.VMEM) for o in outs))


def solution(mesh):
    return jax.shard_map(
        body,
        mesh=mesh,
        in_specs=(
            P("row", "col", None, None),
            P("row", "col", None, None),
            P("col", "row", None, None),
            P("col", None, None),
            P(),
        ),
        out_specs=(P("col", "row", None, None), P("row", "col", None, None), P("col", None, None)),
        check_vma=False,
    )
```

```python
import functools

import jax
import jax.numpy as jnp
from jax import lax
from jax.experimental import pallas as pl
from jax.experimental.pallas import tpu as pltpu
from jax.sharding import PartitionSpec as P

NY = 2
CORES = 2
BF = jnp.bfloat16
F32 = jnp.float32


def kernel(
    n_row, n_col, nq, nf,
    mem_in, anc, low, upp, piv_in,
    low_out, upp_out, diag_out,
    mem, piv, a, lbuf, ubuf, pl_buf, yr, zr, zq, pu, pr, ur, ds, dr, acc, dacc,
    loc, l_s, l_rel, l_r, uy_s, uy_r, uz_s, uz_r, ry_s, ry_r, rz_s, rz_r, rq_s, rq_r,
    pr_s, pr_r, pu_s, pu_r, d_s, d_r,
):
    row = lax.axis_index("row")
    col = lax.axis_index("col")
    nz = n_col // NY
    nx = n_row // CORES
    x, core = row // CORES, row % CORES
    z, y = col // NY, col % NY
    yp = z * NY + (1 - y)
    rb, cb = anc.shape[0], anc.shape[1]
    kr, cs = low.shape[0], low.shape[1]
    rs = upp.shape[1]
    ny_blocks = rs - nq
    nyf = rs - nf
    partner = x * CORES + (1 - core)

    def remote(src, dst, ss, rsem, **where):
        return pltpu.make_async_remote_copy(
            src_ref=src, dst_ref=dst, send_sem=ss, recv_sem=rsem, device_id=where
        )

    ca = pltpu.make_async_copy(anc, a, loc.at[0])
    cl = pltpu.make_async_copy(low, lbuf.at[pl.ds(row * kr, kr)], loc.at[1])
    cu = pltpu.make_async_copy(upp.at[0], ubuf.at[col], loc.at[2])
    cp = pltpu.make_async_copy(piv_in.at[0], piv, loc.at[3])
    cm = pltpu.make_async_copy(mem_in, mem, loc.at[4])
    cm.start()
    cu.start()
    cl.start()
    ca.start()
    cp.start()

    bar = pltpu.get_barrier_semaphore()
    for dx in range(1, n_row):
        pl.semaphore_signal(bar, inc=1, device_id={"row": (row + dx) % n_row})
    pl.semaphore_signal(bar, inc=1, device_id={"col": yp})

    @pl.when(z > 0)
    def _():
        pl.semaphore_signal(bar, inc=1, device_id={"col": col - NY})

    @pl.when(z < nz - 1)
    def _():
        pl.semaphore_signal(bar, inc=1, device_id={"col": col + NY})

    peers = n_row + jnp.where(z > 0, 1, 0) + jnp.where(z < nz - 1, 1, 0)
    pl.semaphore_wait(bar, peers)

    def l_own(r2):
        blk = lbuf.at[pl.ds(row * kr, kr)]
        return remote(blk, blk, l_s.at[r2], l_r.at[row], row=r2)

    def l_recv(r2):
        blk = lbuf.at[pl.ds(r2 * kr, kr)]
        return remote(blk, blk, l_rel.at[r2], l_r.at[r2], row=partner)

    def uy_own(kind):
        part = pl.ds(0, ny_blocks) if kind else pl.ds(ny_blocks, nq)
        return remote(
            ubuf.at[col, part], ubuf.at[col, part], uy_s.at[nz if kind == 0 else z],
            uy_r.at[nz if kind == 0 else z], col=yp,
        )

    def uy_got(kind, zs):
        part = pl.ds(0, ny_blocks) if kind else pl.ds(ny_blocks, nq)
        blk = ubuf.at[zs * NY + (1 - y), part]
        return remote(blk, blk, uy_s.at[zs], uy_r.at[nz if kind == 0 else zs], col=yp)

    def uy_pass(zs):
        blk = ubuf.at[zs * NY + y, pl.ds(0, ny_blocks)]
        return remote(blk, blk, uy_s.at[zs], uy_r.at[zs], col=yp)

    def uz(zs, kind, up):
        if kind == 0:
            blk = ubuf.at[zs * NY + y]
        else:
            blk = ubuf.at[zs * NY + (1 - y), pl.ds(ny_blocks, nq)]
        to = col + NY if up else col - NY
        return remote(blk, blk, uz_s.at[zs, int(up), kind], uz_r.at[zs, kind], col=to)

    def uz_own(up):
        to = col + NY if up else col - NY
        return remote(ubuf.at[col], ubuf.at[col], uz_s.at[z, int(up), 0], uz_r.at[z, 0], col=to)

    def ry(zd, h):
        return remote(
            pl_buf.at[zd * NY + (1 - y), h], yr.at[zd, h], ry_s.at[zd, h], ry_r.at[zd, h], col=yp
        )

    def rz(zd, h, up):
        slot = zd + 1 if up else zd
        to = col + NY if up else col - NY
        return remote(
            pl_buf.at[zd * NY + y, h], zr.at[slot, h], rz_s.at[zd, h], rz_r.at[slot, h], col=to
        )

    def rq(zd, f, up):
        slot = zd + 1 if up else zd
        to = col + NY if up else col - NY
        return remote(
            pl_buf.at[zd * NY + (1 - y), nyf + f], zq.at[slot, f], rq_s.at[zd, f],
            rq_r.at[slot, f], col=to,
        )

    def pr_copy(k):
        return remote(pu.at[k], pr.at[k], pr_s.at[k], pr_r.at[k], row=partner)

    def pu_copy(k):
        return remote(pu.at[k], ur.at[x, k % kr], pu_s.at[k], pu_r.at[x, k % kr], row=k // kr)

    def pu_got(x2, p):
        return remote(
            pu.at[0], ur.at[x2, p], pu_s.at[0], pu_r.at[x2, p], row=x2 * CORES + core
        )

    def keeps(k):
        return (k // kr) % CORES == core

    def leaves(k):
        return k // (kr * CORES) != x

    def d_copy(r2):
        return remote(ds, dr.at[row], d_s.at[r2], d_r.at[row], row=r2)

    def d_got(r2):
        return remote(ds, dr.at[r2], d_s.at[r2], d_r.at[r2], row=r2)

    def d_relay(x2):
        r2 = x2 * CORES + core
        blk = dr.at[r2]
        return remote(blk, blk, d_s.at[x2 * CORES + 1 - core], d_r.at[r2], row=partner)

    def each_dir(fn):
        @pl.when(z > 0)
        def _():
            fn(False)

        @pl.when(z < nz - 1)
        def _():
            fn(True)

    def row_member(k, i):
        m = mem[k, row * rs + i]
        return m >= 0, jnp.clip(m - row * rb, 0, rb - 1)

    def col_member(k, j):
        m = mem[k, col * cs + j]
        return m >= 0, jnp.clip(m - col * cb, 0, cb - 1)

    planes = nz // nx
    edge = jnp.logical_or(z == 0, z == nz - 1)

    def mine(zs):
        return zs // planes == x

    def last_to(up):
        e = nz - 1 if up else 0
        return jnp.where(mine(e), nz - 2 if up else 1, nz - 1 - e)

    def held_back(zs, up):
        return jnp.logical_and(z == (nz - 2 if up else 1), zs == last_to(up))

    def order(i):
        near_half = jnp.where(i % 2 == 0, nz // 2 + i // 2, i // 2)
        dist = jnp.where(mine(z), near_half, i)
        inner_low = jnp.where(i < nz // 2, nz // 2 + i, nz - 1 - i)
        inner_high = jnp.where(i < nz // 2, nz // 2 - 1 - i, i)
        return jnp.where(
            edge, jnp.where(z == 0, dist, nz - 1 - dist),
            jnp.where(2 * x < nx, inner_low, inner_high),
        )

    zero = jnp.zeros((), BF)

    def lower_part(k):
        cols = [col_member(k, j) for j in range(cs)]
        panels = [jnp.where(cols[j][0], lbuf[k, j], zero) for j in range(cs)]

        def one(i, _):
            ok, ri = row_member(k, i)
            tot = None
            for j in range(cs):
                t = jnp.dot(a[ri, cols[j][1]], panels[j], preferred_element_type=F32)
                tot = t if tot is None else tot + t
            pl_buf[k, i] = jnp.where(ok, tot, 0.0).astype(BF)
            return 0

        lax.fori_loop(0, rs, one, 0)

    def upper_part(k):
        rows = [row_member(k, i) for i in range(rs)]

        def one(j, _):
            ok, cj = col_member(k, j)
            tot = None
            for i in range(rs):
                t = jnp.dot(
                    jnp.where(rows[i][0], ubuf[k, i], zero), a[rows[i][1], cj],
                    preferred_element_type=F32,
                )
                tot = t if tot is None else tot + t
            pu[k, j] = jnp.where(ok, tot, 0.0).astype(BF)
            return 0

        lax.fori_loop(0, cs, one, 0)

        @pl.when(jnp.logical_not(keeps(k)))
        def _():
            pr_copy(k).start()

    def finish(k):
        @pl.when(jnp.logical_and(keeps(k), leaves(k)))
        def _():
            pr_copy(k).wait_recv()
            for j in range(cs):
                pu[k, j] = (pu[k, j].astype(F32) + pr[k, j].astype(F32)).astype(BF)
            pu_copy(k).start()

    def lower_group(r2):
        def one(p, _):
            k = r2 * kr + (p + 1 - y) % NY
            lower_part(k)

            @pl.when(k % NY != y)
            def _():
                for h in range(nyf):
                    ry(k // NY, h).start()

            return 0

        lax.fori_loop(0, kr, one, 0)

    def both_groups(x2):
        def one(q, _):
            lower_group(x2 * CORES + jnp.where(2 * x2 >= nx, CORES - 1 - q, q))
            return 0

        lax.fori_loop(0, CORES, one, 0)

    cu.wait()
    uy_own(0).start()
    each_dir(lambda up: uz_own(up).start())
    cl.wait()
    l_own(partner).start()
    for dx in range(1, nx):
        l_own(((x + dx) % nx) * CORES + core).start()
    cm.wait()
    ca.wait()
    l_recv(partner).wait_recv()
    both_groups(x)

    uy_got(0, z).wait_recv()

    def share(zs, up):
        @pl.when(jnp.logical_not(held_back(zs, up)))
        def _():
            uz(zs, 1, up).start()

    each_dir(lambda up: share(z, up))
    upper_part(col)

    def others(fn):
        for dx in range(1, nx):
            fn((x + dx) % nx)

    def relay(x2):
        l_recv(x2 * CORES + core).wait_recv()
        l_recv(x2 * CORES + core).start()

    others(relay)

    def by_side(d, fn):
        @pl.when(z - d >= 0)
        def _():
            fn(z - d, True)

        @pl.when(z + d <= nz - 1)
        def _():
            fn(z + d, False)

    def take(kind):
        def one(zs, up):
            uz(zs, kind, up).wait_recv()

            @pl.when((z < nz - 1) if up else (z > 0))
            def _():
                if kind:
                    share(zs, up)
                else:
                    uz(zs, kind, up).start()

        return one

    by_side(1, take(0))

    def late(x2):
        l_recv(x2 * CORES + 1 - core).wait_recv()
        both_groups(x2)

    others(late)

    @pl.when(jnp.logical_not(edge))
    def _():
        by_side(1, take(1))

    def hand_on(zs):
        @pl.when(zs == z)
        def _():
            uy_own(1).start()

        @pl.when(zs != z)
        def _():
            uy_pass(zs).start()

    def sides(d, fn):
        def one(s, _):
            zs = z + (2 * s - 1) * d

            @pl.when(jnp.logical_and(zs >= 0, zs < nz))
            def _():
                fn(zs)

            return 0

        lax.fori_loop(0, 2, one, 0)

    def near(d):
        sides(d, lambda zs: upper_part(zs * NY + y))

    def near_done(d):
        sides(d, lambda zs: finish(zs * NY + y))

    def across(i):
        zs = order(i)

        @pl.when(jnp.logical_and(edge, zs > z))
        def _():
            uz(zs, 1, False).wait_recv()

        @pl.when(jnp.logical_and(edge, zs < z))
        def _():
            uz(zs, 1, True).wait_recv()

        uy_got(1, zs).wait_recv()
        upper_part(zs * NY + (1 - y))

    def across_done(i):
        finish(order(i) * NY + (1 - y))

    def home():
        k2 = z * NY + (1 - y)
        for f in range(nf):
            each_dir(lambda up: rq(z, f, not up).wait_recv())

            @pl.when(z > 0)
            def _():
                add_to(k2, nyf + f, [zq[z + 1, f]])

            @pl.when(z < nz - 1)
            def _():
                add_to(k2, nyf + f, [zq[z, f]])

            ry(z, nyf + f).start()

    def add_to(k, h, terms):
        tot = pl_buf[k, h].astype(F32)
        for t in terms:
            tot = tot + t.astype(F32)
        pl_buf[k, h] = tot.astype(BF)

    def hop(zd, h, own, waits_y):
        k = zd * NY + (y if own else 1 - y)

        def go(up):
            slot = zd + 1 if up else zd
            step = rz(zd, h, up) if own else rq(zd, h - nyf, up)
            if waits_y:
                ry(zd, h).wait_recv()

            @pl.when((z > 0) if up else (z < nz - 1))
            def _():
                step.wait_recv()
                part = zr[slot, h] if own else zq[slot, h - nyf]
                add_to(k, h, [yr[zd, h], part] if waits_y else [part])

            if waits_y:
                @pl.when((z == 0) if up else (z == nz - 1))
                def _():
                    add_to(k, h, [yr[zd, h]])

            step.start()

        @pl.when(zd > z)
        def _():
            go(True)

        @pl.when(zd < z)
        def _():
            go(False)

    def firsts(zds):
        for f in range(nyf, rs):
            for zd, ok in zds:
                @pl.when(ok)
                def _():
                    hop(zd, f, True, False)
                    hop(zd, f, False, False)

    def seconds(zds, hook=None, close=None):
        def piece(h, _):
            if hook is not None:
                hook(h)
            for zd, ok in zds:
                @pl.when(ok)
                def _():
                    hop(zd, h, True, True)

                if close is not None and zd is zds[0][0]:
                    @pl.when(h == nyf - 1)
                    def _():
                        close()

            return 0

        lax.fori_loop(0, nyf, piece, 0)

    near(1)
    finish(col)

    @pl.when(edge)
    def _():
        def ends(j):
            return [(jnp.where(z == 0, nz - 1 - j, j), j < nz - 1)]

        def opening(j, _):
            firsts(ends(j))
            return 0

        lax.fori_loop(0, 2, opening, 0)
        seconds(ends(0))

        def on(dist):
            hand_on(jnp.where(z == 0, dist, nz - 1 - dist))

        def one(d, _):
            by_side(d, take(0))

            @pl.when(jnp.logical_and(mine(z), d >= nz // 2))
            def _():
                on(d)

                @pl.when(d < nz - 1)
                def _():
                    on(d - nz // 2)

            @pl.when(jnp.logical_not(mine(z)))
            def _():
                @pl.when(d == 2)
                def _():
                    on(0)
                    on(1)

                @pl.when(d < nz - 1)
                def _():
                    on(d)

            near(d)
            near_done(d - 1)
            seconds(ends(d - 1))
            firsts(ends(d))
            return 0

        lax.fori_loop(2, nz, one, 0)
        across(0)
        near_done(nz - 1)
        home()
        hand_on(order(nz - 1))
        across(1)
        across_done(0)

    @pl.when(jnp.logical_not(edge))
    def _():
        def one(d, _):
            by_side(d, take(0))
            by_side(d, take(1))
            near(d)
            near_done(d - 1)
            return 0

        lax.fori_loop(2, nz - 1, one, 0)
        for i in range(nz - 1):
            hand_on(order(i))
        near_done(nz - 2)
        low_half = 2 * z < nz
        short = jnp.where(low_half, z, nz - 1 - z)
        gap = nz - 1 - 2 * short
        spot = nyf - 2

        def pair(s, _):
            s2 = s - gap

            def hook(h):
                now = s == nz - 2 - short

                @pl.when(jnp.logical_and(now, h - spot == 0))
                def _():
                    across(0)

                @pl.when(jnp.logical_and(now, h - spot == 1))
                def _():
                    across(1)

            def close():
                @pl.when(s2 == short - 1)
                def _():
                    @pl.when(z == 1)
                    def _():
                        uz(last_to(False), 1, False).start()

                    @pl.when(z == nz - 2)
                    def _():
                        uz(last_to(True), 1, True).start()

            both = [
                (
                    jnp.where(low_half, s2, nz - 1 - s2),
                    jnp.logical_and(s2 >= 0, s2 < short),
                ),
                (jnp.where(low_half, nz - 1 - s, s), s >= 0),
            ]
            firsts(both)
            seconds(both, hook, close)
            return 0

        lax.fori_loop(0, nz - 1 - short, pair, 0)
        home()
        hand_on(order(nz - 1))
        across_done(0)

    across_done(1)

    def rest(i, _):
        across(i)

        @pl.when(i > 2)
        def _():
            across_done(i - 1)

        return 0

    lax.fori_loop(2, nz - 1, rest, 0)

    def final(h, _):
        ry(z, h).wait_recv()
        acc[h] = pl_buf[col, h].astype(F32) + yr[z, h].astype(F32)

        @pl.when(z > 0)
        def _():
            rz(z, h, True).wait_recv()
            acc[h] = acc[h] + zr[z + 1, h].astype(F32)

        @pl.when(z < nz - 1)
        def _():
            rz(z, h, False).wait_recv()
            acc[h] = acc[h] + zr[z, h].astype(F32)

        low_out[0, h] = (-acc[h]).astype(BF)
        return 0

    lax.fori_loop(0, rs, final, 0)
    tot = None
    for i in range(rs):
        t = jnp.dot(
            jnp.where(row_member(col, i)[0], ubuf[col, i], zero), low_out[0, i],
            preferred_element_type=F32,
        )
        tot = t if tot is None else tot + t
    dacc[...] = tot
    ds[...] = tot.astype(BF)
    others(lambda x2: d_copy(x2 * CORES + core).start())
    d_copy(partner).start()

    across_done(nz - 2)
    across(nz - 1)
    across_done(nz - 1)


    def d_pass(x2):
        d_got(x2 * CORES + core).wait_recv()
        d_relay(x2).start()

    def d_add(r2):
        dacc[...] = dacc[...] + dr[r2].astype(F32)

    others(d_pass)
    d_got(partner).wait_recv()
    d_add(partner)

    def d_add_chip(x2):
        d_add(x2 * CORES + core)
        d_got(x2 * CORES + 1 - core).wait_recv()
        d_add(x2 * CORES + 1 - core)

    others(d_add_chip)
    cp.wait()
    diag_out[0] = piv[...] - dacc[...]

    for p in range(kr):
        pr_copy(row * kr + p).wait_recv()
        for j in range(cs):
            acc[p * cs + j] = pu[row * kr + p, j].astype(F32) + pr[row * kr + p, j].astype(F32)

    def pu_add(x2):
        for p in range(kr):
            pu_got(x2, p).wait_recv()
            for j in range(cs):
                acc[p * cs + j] = acc[p * cs + j] + ur[x2, p, j].astype(F32)

    others(pu_add)
    for p in range(kr):
        for j in range(cs):
            upp_out[p, j] = (-acc[p * cs + j]).astype(BF)

    l_own(partner).wait_send()
    for dx in range(1, nx):
        r2 = ((x + dx) % nx) * CORES + core
        l_own(r2).wait_send()
        l_recv(r2).wait_send()
    uy_own(0).wait_send()
    uy_own(1).wait_send()

    def own_done(up):
        uz_own(up).wait_send()
        uz(z, 1, up).wait_send()

    each_dir(own_done)

    def passed(zs, up):
        uy_pass(zs).wait_send()

        @pl.when((z < nz - 1) if up else (z > 0))
        def _():
            for kind in range(2):
                uz(zs, kind, up).wait_send()

    for d in range(1, nz):
        by_side(d, passed)

    def sums_done(zd, _):
        for h in range(nyf):
            ry(zd, h).wait_send()

        def along(up):
            for h in range(rs):
                rz(zd, h, up).wait_send()
            for f in range(nf):
                rq(zd, f, up).wait_send()

        @pl.when(zd > z)
        def _():
            along(True)

        @pl.when(zd < z)
        def _():
            along(False)

        return 0

    lax.fori_loop(0, nz, sums_done, 0)
    for f in range(nf):
        ry(z, nyf + f).wait_send()

    def parts_done(k, _):
        @pl.when(jnp.logical_not(keeps(k)))
        def _():
            pr_copy(k).wait_send()

        @pl.when(jnp.logical_and(keeps(k), leaves(k)))
        def _():
            pu_copy(k).wait_send()

        return 0

    lax.fori_loop(0, n_col, parts_done, 0)
    d_copy(partner).wait_send()

    def d_done(x2):
        d_copy(x2 * CORES + core).wait_send()
        d_relay(x2).wait_send()

    others(d_done)


def hand_over(*refs):
    sems = refs[-1]
    copies = [
        pltpu.make_async_copy(src, dst, sems.at[i])
        for i, (src, dst) in enumerate(zip(refs[:3], refs[3:6]))
    ]
    for c in copies:
        c.start()
    for c in copies:
        c.wait()


def body(ancestor_inv, lower_panel, upper_panel, pivot_inv, members):
    n_col = lax.axis_size("col")
    n_row = lax.axis_size("row")
    side = ancestor_inv.shape[2]
    rb, cb = ancestor_inv.shape[:2]
    kr, cs = lower_panel.shape[:2]
    per_col, rs = upper_panel.shape[:2]
    level = members.shape[0]
    nz = n_col // NY
    assert per_col == 1 and level == n_col and kr == NY and nz == n_row and rs >= 4
    nf = max(1, rs // 4)
    nq = rs // 2
    blk = (side, side)
    dma = pltpu.SemaphoreType.DMA
    vmem = pl.BlockSpec(memory_space=pltpu.VMEM)
    hbm = pl.BlockSpec(memory_space=pltpu.HBM)
    outs = pl.pallas_call(
        functools.partial(kernel, n_row, n_col, nq, nf),
        out_shape=(
            pltpu.VMEM((per_col, rs) + blk, BF),
            pltpu.VMEM((kr, cs) + blk, BF),
            pltpu.VMEM((per_col,) + blk, F32),
        ),
        in_specs=[hbm] * 5,
        out_specs=(vmem, vmem, vmem),
        scratch_shapes=[
            pltpu.SMEM(members.shape, jnp.int32),
            pltpu.VMEM(blk, F32),
            pltpu.VMEM((rb, cb) + blk, BF),
            pltpu.VMEM((level, cs) + blk, BF),
            pltpu.VMEM((n_col, rs) + blk, BF),
            pltpu.VMEM((n_col, rs) + blk, BF),
            pltpu.VMEM((nz, rs) + blk, BF),
            pltpu.VMEM((nz + 1, rs) + blk, BF),
            pltpu.VMEM((nz + 1, nf) + blk, BF),
            pltpu.VMEM((level, cs) + blk, BF),
            pltpu.VMEM((level, cs) + blk, BF),
            pltpu.VMEM((n_row // CORES, kr, cs) + blk, BF),
            pltpu.VMEM(blk, BF),
            pltpu.VMEM((n_row,) + blk, BF),
            pltpu.VMEM((max(rs, kr * cs),) + blk, F32),
            pltpu.VMEM(blk, F32),
            dma((5,)), dma((n_row,)), dma((n_row,)), dma((n_row,)),
            dma((nz + 1,)), dma((nz + 1,)), dma((nz, 2, 2)), dma((nz, 2)),
            dma((nz, rs)), dma((nz, rs)), dma((nz, rs)), dma((nz + 1, rs)),
            dma((nz, nf)), dma((nz + 1, nf)), dma((n_col,)), dma((n_col,)),
            dma((n_col,)), dma((n_row // CORES, kr)), dma((n_row,)), dma((n_row,)),
        ],
        compiler_params=pltpu.CompilerParams(
            collective_id=0, has_side_effects=True, vmem_limit_bytes=60 * 1024 * 1024
        ),
    )(members, ancestor_inv, lower_panel, upper_panel, pivot_inv)
    return pl.pallas_call(
        hand_over,
        out_shape=tuple(jax.ShapeDtypeStruct(o.shape, o.dtype) for o in outs),
        in_specs=[vmem] * 3,
        out_specs=(hbm,) * 3,
        scratch_shapes=[dma((3,))],
    )(*(pltpu.with_memory_space_constraint(o, pltpu.VMEM) for o in outs))


def solution(mesh):
    return jax.shard_map(
        body,
        mesh=mesh,
        in_specs=(
            P("row", "col", None, None),
            P("row", "col", None, None),
            P("col", "row", None, None),
            P("col", None, None),
            P(),
        ),
        out_specs=(P("col", "row", None, None), P("row", "col", None, None), P("col", None, None)),
        check_vma=False,
    )
```

```python
import functools

import jax
import jax.numpy as jnp
from jax import lax
from jax.experimental import pallas as pl
from jax.experimental.pallas import tpu as pltpu
from jax.sharding import PartitionSpec as P

NY = 2
CORES = 2
BF = jnp.bfloat16
F32 = jnp.float32


def kernel(
    n_row, n_col, nq, nf,
    mem_in, anc, low, upp, piv_in,
    low_out, upp_out, diag_out,
    mem, piv, a, lbuf, ubuf, pl_buf, yr, zr, zq, pu, pr, ur, ds, dr, acc, dacc,
    loc, sent, l_r, uy_r, uz_r, ry_r, rz_r, rq_r, pr_r, pu_r, d_r,
):
    row = lax.axis_index("row")
    col = lax.axis_index("col")
    nz = n_col // NY
    nx = n_row // CORES
    x, core = row // CORES, row % CORES
    z, y = col // NY, col % NY
    yp = z * NY + (1 - y)
    rb, cb = anc.shape[0], anc.shape[1]
    kr, cs = low.shape[0], low.shape[1]
    rs = upp.shape[1]
    ny_blocks = rs - nq
    nyf = rs - nf
    partner = x * CORES + (1 - core)

    def remote(src, dst, ss, rsem, **where):
        return pltpu.make_async_remote_copy(
            src_ref=src, dst_ref=dst, send_sem=ss, recv_sem=rsem, device_id=where
        )

    ca = pltpu.make_async_copy(anc, a, loc.at[0])
    cl = pltpu.make_async_copy(low, lbuf.at[pl.ds(row * kr, kr)], loc.at[1])
    cu = pltpu.make_async_copy(upp.at[0], ubuf.at[col], loc.at[2])
    cp = pltpu.make_async_copy(piv_in.at[0], piv, loc.at[3])
    cm = pltpu.make_async_copy(mem_in, mem, loc.at[4])
    cm.start()
    cu.start()
    cl.start()
    ca.start()
    cp.start()

    bar = pltpu.get_barrier_semaphore()
    for dx in range(1, n_row):
        pl.semaphore_signal(bar, inc=1, device_id={"row": (row + dx) % n_row})
    pl.semaphore_signal(bar, inc=1, device_id={"col": yp})

    @pl.when(z > 0)
    def _():
        pl.semaphore_signal(bar, inc=1, device_id={"col": col - NY})

    @pl.when(z < nz - 1)
    def _():
        pl.semaphore_signal(bar, inc=1, device_id={"col": col + NY})

    peers = n_row + jnp.where(z > 0, 1, 0) + jnp.where(z < nz - 1, 1, 0)
    pl.semaphore_wait(bar, peers)

    L_S, UY_S, RY_S, RH_S, RZ_S, RQ_S, PR_S, PU_S, D_S, UZ_S = range(10)

    def l_own(r2):
        blk = lbuf.at[pl.ds(row * kr, kr)]
        return remote(blk, blk, sent.at[L_S], l_r.at[row], row=r2)

    def l_recv(r2):
        blk = lbuf.at[pl.ds(r2 * kr, kr)]
        return remote(blk, blk, sent.at[L_S], l_r.at[r2], row=partner)

    def uy(k, late, rsem):
        part = pl.ds(0, ny_blocks) if late else pl.ds(ny_blocks, nq)
        blk = ubuf.at[k, part]
        return remote(blk, blk, sent.at[UY_S], uy_r.at[rsem], col=yp)

    def uy_own(kind):
        return uy(col, kind == 1, z if kind else nz)

    def uy_got(kind, zs):
        return uy(zs * NY + (1 - y), kind == 1, zs if kind else nz)

    def uy_pass(zs):
        return uy(zs * NY + y, True, zs)

    def uz(zs, kind, up):
        k = zs * NY + (1 - y if kind == 2 else y)
        blk = ubuf.at[k, pl.ds(0, ny_blocks) if kind == 0 else pl.ds(ny_blocks, nq)]
        to = col + NY if up else col - NY
        return remote(blk, blk, sent.at[UZ_S + kind], uz_r.at[zs, kind], col=to)

    def ry_at(zd, h, ssem):
        return remote(
            pl_buf.at[zd * NY + (1 - y), h], yr.at[zd, h], sent.at[ssem], ry_r.at[zd, h], col=yp
        )

    def ry(zd, h):
        return ry_at(zd, h, RY_S)

    def rz(zd, h, up):
        slot = zd + 1 if up else zd
        to = col + NY if up else col - NY
        return remote(
            pl_buf.at[zd * NY + y, h], zr.at[slot, h], sent.at[RZ_S], rz_r.at[slot, h], col=to
        )

    def rq(zd, f, up):
        slot = zd + 1 if up else zd
        to = col + NY if up else col - NY
        return remote(
            pl_buf.at[zd * NY + (1 - y), nyf + f], zq.at[slot, f], sent.at[RQ_S],
            rq_r.at[slot, f], col=to,
        )

    def pr_copy(k):
        return remote(pu.at[k], pr.at[k], sent.at[PR_S], pr_r.at[k], row=partner)

    def pu_copy(k):
        return remote(pu.at[k], ur.at[x, k % kr], sent.at[PU_S], pu_r.at[x, k % kr], row=k // kr)

    def pu_got(x2, p):
        return remote(
            pu.at[0], ur.at[x2, p], sent.at[PU_S], pu_r.at[x2, p], row=x2 * CORES + core
        )

    def keeps(k):
        return (k // kr) % CORES == core

    def leaves(k):
        return k // (kr * CORES) != x

    def d_copy(r2):
        return remote(ds, dr.at[row], sent.at[D_S], d_r.at[row], row=r2)

    def d_got(r2):
        return remote(ds, dr.at[r2], sent.at[D_S], d_r.at[r2], row=r2)

    def d_relay(x2):
        r2 = x2 * CORES + core
        blk = dr.at[r2]
        return remote(blk, blk, sent.at[D_S], d_r.at[r2], row=partner)

    def each_dir(fn):
        @pl.when(z > 0)
        def _():
            fn(False)

        @pl.when(z < nz - 1)
        def _():
            fn(True)

    def row_member(k, i):
        m = mem[k, row * rs + i]
        return m >= 0, jnp.clip(m - row * rb, 0, rb - 1)

    def col_member(k, j):
        m = mem[k, col * cs + j]
        return m >= 0, jnp.clip(m - col * cb, 0, cb - 1)

    planes = nz // nx
    edge = jnp.logical_or(z == 0, z == nz - 1)

    def mine(zs):
        return zs // planes == x

    def last_to(up):
        e = nz - 1 if up else 0
        return jnp.where(mine(e), nz - 2 if up else 1, nz - 1 - e)

    def held_back(zs, up):
        return jnp.logical_and(z == (nz - 2 if up else 1), zs == last_to(up))

    def order(i):
        near_half = jnp.where(i % 2 == 0, nz // 2 + i // 2, i // 2)
        dist = jnp.where(mine(z), near_half, i)
        inner_low = jnp.where(i < nz // 2, nz // 2 + i, nz - 1 - i)
        inner_high = jnp.where(i < nz // 2, nz // 2 - 1 - i, i)
        return jnp.where(
            edge, jnp.where(z == 0, dist, nz - 1 - dist),
            jnp.where(2 * x < nx, inner_low, inner_high),
        )

    zero = jnp.zeros((), BF)

    def lower_part(k):
        cols = [col_member(k, j) for j in range(cs)]
        panels = [jnp.where(cols[j][0], lbuf[k, j], zero) for j in range(cs)]

        def one(i, _):
            ok, ri = row_member(k, i)
            tot = None
            for j in range(cs):
                t = jnp.dot(a[ri, cols[j][1]], panels[j], preferred_element_type=F32)
                tot = t if tot is None else tot + t
            pl_buf[k, i] = jnp.where(ok, tot, 0.0).astype(BF)
            return 0

        lax.fori_loop(0, rs, one, 0)

    def upper_part(k):
        rows = [row_member(k, i) for i in range(rs)]

        def one(j, _):
            ok, cj = col_member(k, j)
            tot = None
            for i in range(rs):
                t = jnp.dot(
                    jnp.where(rows[i][0], ubuf[k, i], zero), a[rows[i][1], cj],
                    preferred_element_type=F32,
                )
                tot = t if tot is None else tot + t
            pu[k, j] = jnp.where(ok, tot, 0.0).astype(BF)
            return 0

        lax.fori_loop(0, cs, one, 0)

        @pl.when(jnp.logical_not(keeps(k)))
        def _():
            pr_copy(k).start()

    def finish(k):
        @pl.when(jnp.logical_and(keeps(k), leaves(k)))
        def _():
            pr_copy(k).wait_recv()
            for j in range(cs):
                pu[k, j] = (pu[k, j].astype(F32) + pr[k, j].astype(F32)).astype(BF)
            pu_copy(k).start()

    def lower_group(r2):
        def one(p, _):
            k = r2 * kr + (p + 1 - y) % NY
            lower_part(k)

            @pl.when(k % NY != y)
            def _():
                for h in range(nyf):
                    ry(k // NY, h).start()

            return 0

        lax.fori_loop(0, kr, one, 0)

    def both_groups(x2):
        def one(q, _):
            lower_group(x2 * CORES + jnp.where(2 * x2 >= nx, CORES - 1 - q, q))
            return 0

        lax.fori_loop(0, CORES, one, 0)

    cu.wait()
    uy_own(0).start()
    each_dir(lambda up: uz(z, 0, up).start())
    each_dir(lambda up: uz(z, 1, up).start())
    cl.wait()
    l_own(partner).start()
    for dx in range(1, nx):
        l_own(((x + dx) % nx) * CORES + core).start()
    cm.wait()
    ca.wait()
    l_recv(partner).wait_recv()
    both_groups(x)

    uy_got(0, z).wait_recv()

    def share(zs, up):
        @pl.when(jnp.logical_not(held_back(zs, up)))
        def _():
            uz(zs, 2, up).start()

    each_dir(lambda up: share(z, up))
    upper_part(col)

    def others(fn):
        for dx in range(1, nx):
            fn((x + dx) % nx)

    def relay(x2):
        l_recv(x2 * CORES + core).wait_recv()
        l_recv(x2 * CORES + core).start()

    def by_side(d, fn):
        @pl.when(z - d >= 0)
        def _():
            fn(z - d, True)

        @pl.when(z + d <= nz - 1)
        def _():
            fn(z + d, False)

    def take(kind):
        def one(zs, up):
            uz(zs, kind, up).wait_recv()

            @pl.when((z < nz - 1) if up else (z > 0))
            def _():
                if kind == 2:
                    share(zs, up)
                else:
                    uz(zs, kind, up).start()

        return one

    by_side(1, take(0))
    others(relay)
    by_side(1, take(1))

    def late(x2):
        l_recv(x2 * CORES + 1 - core).wait_recv()
        both_groups(x2)

    others(late)

    @pl.when(jnp.logical_not(edge))
    def _():
        by_side(1, take(2))

    def hand_on(zs):
        @pl.when(zs == z)
        def _():
            uy_own(1).start()

        @pl.when(zs != z)
        def _():
            uy_pass(zs).start()

    def sides(d, fn):
        def one(s, _):
            zs = z + (2 * s - 1) * d

            @pl.when(jnp.logical_and(zs >= 0, zs < nz))
            def _():
                fn(zs)

            return 0

        lax.fori_loop(0, 2, one, 0)

    def near(d):
        sides(d, lambda zs: upper_part(zs * NY + y))

    def near_done(d):
        sides(d, lambda zs: finish(zs * NY + y))

    def across(i):
        zs = order(i)

        @pl.when(jnp.logical_and(edge, zs > z))
        def _():
            uz(zs, 2, False).wait_recv()

        @pl.when(jnp.logical_and(edge, zs < z))
        def _():
            uz(zs, 2, True).wait_recv()

        uy_got(1, zs).wait_recv()
        upper_part(zs * NY + (1 - y))

    def across_done(i):
        finish(order(i) * NY + (1 - y))

    def home():
        k2 = z * NY + (1 - y)
        for f in range(nf):
            each_dir(lambda up: rq(z, f, not up).wait_recv())

            @pl.when(z > 0)
            def _():
                add_to(k2, nyf + f, [zq[z + 1, f]])

            @pl.when(z < nz - 1)
            def _():
                add_to(k2, nyf + f, [zq[z, f]])

            ry_at(z, nyf + f, RH_S).start()

    def add_to(k, h, terms):
        tot = pl_buf[k, h].astype(F32)
        for t in terms:
            tot = tot + t.astype(F32)
        pl_buf[k, h] = tot.astype(BF)

    def hop(zd, h, own, waits_y):
        k = zd * NY + (y if own else 1 - y)

        def go(up):
            slot = zd + 1 if up else zd
            step = rz(zd, h, up) if own else rq(zd, h - nyf, up)
            if waits_y:
                ry(zd, h).wait_recv()

            @pl.when((z > 0) if up else (z < nz - 1))
            def _():
                step.wait_recv()
                part = zr[slot, h] if own else zq[slot, h - nyf]
                add_to(k, h, [yr[zd, h], part] if waits_y else [part])

            if waits_y:
                @pl.when((z == 0) if up else (z == nz - 1))
                def _():
                    add_to(k, h, [yr[zd, h]])

            step.start()

        @pl.when(zd > z)
        def _():
            go(True)

        @pl.when(zd < z)
        def _():
            go(False)

    def firsts(zds):
        for f in range(nyf, rs):
            for zd, ok in zds:
                @pl.when(ok)
                def _():
                    hop(zd, f, True, False)
                    hop(zd, f, False, False)

    def seconds(zds, hook=None, close=None):
        def piece(h, _):
            if hook is not None:
                hook(h)
            for zd, ok in zds:
                @pl.when(ok)
                def _():
                    hop(zd, h, True, True)

                if close is not None and zd is zds[0][0]:
                    @pl.when(h == nyf - 1)
                    def _():
                        close()

            return 0

        lax.fori_loop(0, nyf, piece, 0)

    near(1)
    finish(col)

    @pl.when(edge)
    def _():
        def ends(j):
            return [(jnp.where(z == 0, nz - 1 - j, j), j < nz - 1)]

        def opening(j, _):
            firsts(ends(j))
            return 0

        lax.fori_loop(0, 2, opening, 0)
        seconds(ends(0))

        def on(dist):
            hand_on(jnp.where(z == 0, dist, nz - 1 - dist))

        def one(d, _):
            by_side(d, take(0))

            @pl.when(jnp.logical_and(mine(z), d >= nz // 2))
            def _():
                on(d)

                @pl.when(d < nz - 1)
                def _():
                    on(d - nz // 2)

            @pl.when(jnp.logical_not(mine(z)))
            def _():
                @pl.when(d == 2)
                def _():
                    on(0)
                    on(1)

                @pl.when(d < nz - 1)
                def _():
                    on(d)

            by_side(d, take(1))
            near(d)
            near_done(d - 1)
            seconds(ends(d - 1))
            firsts(ends(d))
            return 0

        lax.fori_loop(2, nz, one, 0)
        across(0)
        near_done(nz - 1)
        home()
        hand_on(order(nz - 1))
        across(1)
        across_done(0)

    @pl.when(jnp.logical_not(edge))
    def _():
        low_half = 2 * z < nz
        short = jnp.where(low_half, z, nz - 1 - z)

        def one(d, _):
            by_side(d, take(0))
            by_side(d, take(1))

            @pl.when(d == nz - 2)
            def _():
                firsts([(jnp.where(low_half, nz - 1, 0), d > 0)])

            by_side(d, take(2))
            near(d)
            near_done(d - 1)
            return 0

        lax.fori_loop(2, nz - 1, one, 0)
        for i in range(nz - 1):
            hand_on(order(i))
        gap = nz - 1 - 2 * short
        spot = nyf - 2

        def pair(s, _):
            s2 = s - gap

            def hook(h):
                now = s == nz - 2 - short

                @pl.when(jnp.logical_and(now, h - spot == 0))
                def _():
                    near_done(nz - 2)
                    across(0)

                @pl.when(jnp.logical_and(now, h - spot == 1))
                def _():
                    across(1)

            def close():
                @pl.when(s2 == short - 1)
                def _():
                    @pl.when(z == 1)
                    def _():
                        uz(last_to(False), 2, False).start()

                    @pl.when(z == nz - 2)
                    def _():
                        uz(last_to(True), 2, True).start()

            both = [
                (
                    jnp.where(low_half, s2, nz - 1 - s2),
                    jnp.logical_and(s2 >= 0, s2 < short),
                ),
                (jnp.where(low_half, nz - 1 - s, s), s >= 0),
            ]
            firsts([both[0], (both[1][0], s > 0)])
            seconds(both, hook, close)
            return 0

        lax.fori_loop(0, nz - 1 - short, pair, 0)
        home()
        hand_on(order(nz - 1))
        across_done(0)

    across_done(1)

    def rest(i, _):
        across(i)

        @pl.when(i > 2)
        def _():
            across_done(i - 1)

        return 0

    lax.fori_loop(2, nz - 1, rest, 0)

    def final(h, _):
        ry(z, h).wait_recv()
        acc[h] = pl_buf[col, h].astype(F32) + yr[z, h].astype(F32)

        @pl.when(z > 0)
        def _():
            rz(z, h, True).wait_recv()
            acc[h] = acc[h] + zr[z + 1, h].astype(F32)

        @pl.when(z < nz - 1)
        def _():
            rz(z, h, False).wait_recv()
            acc[h] = acc[h] + zr[z, h].astype(F32)

        low_out[0, h] = (-acc[h]).astype(BF)
        return 0

    lax.fori_loop(0, rs, final, 0)
    tot = None
    for i in range(rs):
        t = jnp.dot(
            jnp.where(row_member(col, i)[0], ubuf[col, i], zero), low_out[0, i],
            preferred_element_type=F32,
        )
        tot = t if tot is None else tot + t
    dacc[...] = tot
    ds[...] = tot.astype(BF)
    others(lambda x2: d_copy(x2 * CORES + core).start())
    d_copy(partner).start()

    across_done(nz - 2)

    def d_pass(x2):
        d_got(x2 * CORES + core).wait_recv()
        d_relay(x2).start()

    @pl.when(edge)
    def _():
        others(d_pass)

    across(nz - 1)
    across_done(nz - 1)
    for p in range(kr):
        pr_copy(row * kr + p).wait_recv()
        for j in range(cs):
            acc[p * cs + j] = pu[row * kr + p, j].astype(F32) + pr[row * kr + p, j].astype(F32)

    def pu_add(x2):
        for p in range(kr):
            pu_got(x2, p).wait_recv()
            for j in range(cs):
                acc[p * cs + j] = acc[p * cs + j] + ur[x2, p, j].astype(F32)

    others(pu_add)
    for p in range(kr):
        for j in range(cs):
            upp_out[p, j] = (-acc[p * cs + j]).astype(BF)

    def all_sent(ref, which):
        pltpu.make_async_copy(ref, ref, sent.at[which]).wait()

    for kind in range(3):
        @pl.when(edge)
        def _():
            all_sent(ubuf.at[pl.ds(0, 1), pl.ds(0, nq)], UZ_S + kind)

        @pl.when(jnp.logical_not(edge))
        def _():
            all_sent(ubuf.at[pl.ds(0, nz + 1), pl.ds(0, nq)], UZ_S + kind)

    all_sent(lbuf.at[pl.ds(0, kr * (2 * nx - 1))], L_S)
    all_sent(ubuf.at[pl.ds(0, nz + 1), pl.ds(0, nq)], UY_S)
    all_sent(pl_buf.at[pl.ds(0, nz), pl.ds(0, nyf)], RY_S)
    all_sent(pl_buf.at[pl.ds(0, 1), pl.ds(0, nf)], RH_S)
    all_sent(pl_buf.at[pl.ds(0, nz - 1)], RZ_S)
    all_sent(pl_buf.at[pl.ds(0, nz - 1), pl.ds(0, nf)], RQ_S)
    all_sent(pu.at[pl.ds(0, n_col // CORES)], PR_S)
    all_sent(pu.at[pl.ds(0, kr * (nx - 1))], PU_S)

    @pl.when(jnp.logical_not(edge))
    def _():
        others(d_pass)

    def d_add(r2):
        dacc[...] = dacc[...] + dr[r2].astype(F32)

    d_got(partner).wait_recv()
    d_add(partner)

    def d_add_chip(x2):
        d_add(x2 * CORES + core)
        d_got(x2 * CORES + 1 - core).wait_recv()
        d_add(x2 * CORES + 1 - core)

    others(d_add_chip)
    cp.wait()
    diag_out[0] = piv[...] - dacc[...]
    all_sent(dr.at[pl.ds(0, 2 * nx - 1)], D_S)


def hand_over(*refs):
    sems = refs[-1]
    copies = [
        pltpu.make_async_copy(src, dst, sems.at[i])
        for i, (src, dst) in enumerate(zip(refs[:3], refs[3:6]))
    ]
    for c in copies:
        c.start()
    for c in copies:
        c.wait()


def body(ancestor_inv, lower_panel, upper_panel, pivot_inv, members):
    n_col = lax.axis_size("col")
    n_row = lax.axis_size("row")
    side = ancestor_inv.shape[2]
    rb, cb = ancestor_inv.shape[:2]
    kr, cs = lower_panel.shape[:2]
    per_col, rs = upper_panel.shape[:2]
    level = members.shape[0]
    nz = n_col // NY
    assert per_col == 1 and level == n_col and kr == NY and nz == n_row and rs >= 4 and rs % 2 == 0
    nf = max(1, rs // 4)
    nq = rs // 2
    blk = (side, side)
    dma = pltpu.SemaphoreType.DMA
    vmem = pl.BlockSpec(memory_space=pltpu.VMEM)
    hbm = pl.BlockSpec(memory_space=pltpu.HBM)
    outs = pl.pallas_call(
        functools.partial(kernel, n_row, n_col, nq, nf),
        out_shape=(
            pltpu.VMEM((per_col, rs) + blk, BF),
            pltpu.VMEM((kr, cs) + blk, BF),
            pltpu.VMEM((per_col,) + blk, F32),
        ),
        in_specs=[hbm] * 5,
        out_specs=(vmem, vmem, vmem),
        scratch_shapes=[
            pltpu.SMEM(members.shape, jnp.int32),
            pltpu.VMEM(blk, F32),
            pltpu.VMEM((rb, cb) + blk, BF),
            pltpu.VMEM((level, cs) + blk, BF),
            pltpu.VMEM((n_col, rs) + blk, BF),
            pltpu.VMEM((n_col, rs) + blk, BF),
            pltpu.VMEM((nz, rs) + blk, BF),
            pltpu.VMEM((nz + 1, rs) + blk, BF),
            pltpu.VMEM((nz + 1, nf) + blk, BF),
            pltpu.VMEM((level, cs) + blk, BF),
            pltpu.VMEM((level, cs) + blk, BF),
            pltpu.VMEM((n_row // CORES, kr, cs) + blk, BF),
            pltpu.VMEM(blk, BF),
            pltpu.VMEM((n_row,) + blk, BF),
            pltpu.VMEM((max(rs, kr * cs),) + blk, F32),
            pltpu.VMEM(blk, F32),
            dma((5,)), dma((12,)), dma((n_row,)), dma((nz + 1,)), dma((nz, 3)),
            dma((nz, rs)), dma((nz + 1, rs)), dma((nz + 1, nf)), dma((n_col,)),
            dma((n_row // CORES, kr)), dma((n_row,)),
        ],
        compiler_params=pltpu.CompilerParams(
            collective_id=0, has_side_effects=True, vmem_limit_bytes=60 * 1024 * 1024
        ),
    )(members, ancestor_inv, lower_panel, upper_panel, pivot_inv)
    return pl.pallas_call(
        hand_over,
        out_shape=tuple(jax.ShapeDtypeStruct(o.shape, o.dtype) for o in outs),
        in_specs=[vmem] * 3,
        out_specs=(hbm,) * 3,
        scratch_shapes=[dma((3,))],
    )(*(pltpu.with_memory_space_constraint(o, pltpu.VMEM) for o in outs))


def solution(mesh):
    return jax.shard_map(
        body,
        mesh=mesh,
        in_specs=(
            P("row", "col", None, None),
            P("row", "col", None, None),
            P("col", "row", None, None),
            P("col", None, None),
            P(),
        ),
        out_specs=(P("col", "row", None, None), P("row", "col", None, None), P("col", None, None)),
        check_vma=False,
    )
```

```python
import functools

import jax
import jax.numpy as jnp
from jax import lax
from jax.experimental import pallas as pl
from jax.experimental.pallas import tpu as pltpu
from jax.sharding import PartitionSpec as P

NY = 2
CORES = 2
BF = jnp.bfloat16
F32 = jnp.float32


def kernel(
    n_row, n_col, nq, nf, pz, nyp, py,
    mem_in, anc, low, upp, piv_in,
    low_out, upp_out, diag_out,
    mem, piv, a, lbuf, ubuf, pl_buf, yr, zr, zq, pu, pr, ur, ds, dr, acc, dacc,
    loc, sent, l_r, uy_r, uz_r, ry_r, rh_r, rz_r, rf_r, rq_r,
    pr_r, pu_r, d_r,
):
    row = lax.axis_index("row")
    col = lax.axis_index("col")
    nz = n_col // NY
    nx = n_row // CORES
    x, core = row // CORES, row % CORES
    z, y = col // NY, col % NY
    yp = z * NY + (1 - y)
    rb, cb = anc.shape[0], anc.shape[1]
    kr, cs = low.shape[0], low.shape[1]
    side = low.shape[2]
    rows = upp.shape[1]
    rs = rows // side
    ny = rows - nq
    yf = nyp * py
    partner = x * CORES + (1 - core)

    def remote(src, dst, ss, rsem, **where):
        return pltpu.make_async_remote_copy(
            src_ref=src, dst_ref=dst, send_sem=ss, recv_sem=rsem, device_id=where
        )

    ca = pltpu.make_async_copy(anc, a, loc.at[0])
    cl = pltpu.make_async_copy(low, lbuf.at[pl.ds(row * kr, kr)], loc.at[1])
    cu = pltpu.make_async_copy(upp.at[0], ubuf.at[col], loc.at[2])
    cp = pltpu.make_async_copy(piv_in.at[0], piv, loc.at[3])
    cm = pltpu.make_async_copy(mem_in, mem, loc.at[4])
    cm.start()
    cu.start()
    cl.start()
    ca.start()
    cp.start()

    bar = pltpu.get_barrier_semaphore()
    for dx in range(1, n_row):
        pl.semaphore_signal(bar, inc=1, device_id={"row": (row + dx) % n_row})
    pl.semaphore_signal(bar, inc=1, device_id={"col": yp})

    @pl.when(z > 0)
    def _():
        pl.semaphore_signal(bar, inc=1, device_id={"col": col - NY})

    @pl.when(z < nz - 1)
    def _():
        pl.semaphore_signal(bar, inc=1, device_id={"col": col + NY})

    peers = n_row + jnp.where(z > 0, 1, 0) + jnp.where(z < nz - 1, 1, 0)
    pl.semaphore_wait(bar, peers)

    L_S, UA_S, UY_S, RY_S, RH_S, RZ_S, RQ_S, PR_S, PU_S, D_S, UZ_S = range(11)

    def l_own(r2):
        blk = lbuf.at[pl.ds(row * kr, kr)]
        return remote(blk, blk, sent.at[L_S], l_r.at[row], row=r2)

    def l_recv(r2):
        blk = lbuf.at[pl.ds(r2 * kr, kr)]
        return remote(blk, blk, sent.at[L_S], l_r.at[r2], row=partner)

    def uy(k, late, rsem):
        part = pl.ds(0, ny) if late else pl.ds(ny, nq)
        blk = ubuf.at[k, part]
        return remote(blk, blk, sent.at[UY_S if late else UA_S], uy_r.at[rsem], col=yp)

    def uy_own(kind):
        return uy(col, kind == 1, z if kind else nz)

    def uy_got(kind, zs):
        return uy(zs * NY + (1 - y), kind == 1, zs if kind else nz)

    def uy_pass(zs):
        return uy(zs * NY + y, True, zs)

    def uz(zs, kind, up):
        k = zs * NY + (1 - y if kind == 2 else y)
        blk = ubuf.at[k, pl.ds(0, ny) if kind == 0 else pl.ds(ny, nq)]
        to = col + NY if up else col - NY
        return remote(blk, blk, sent.at[UZ_S + kind], uz_r.at[zs, kind], col=to)

    half = side // 2
    nh = nyp // 2

    def ypart(h):
        return (
            pl.ds(pl.multiple_of((h % nh) * (2 * py), 16), 2 * py),
            pl.ds(pl.multiple_of((h // nh) * half, half), half),
        )

    def zrows(f, base=yf):
        return pl.ds(pl.multiple_of(base + f * pz, 16), pz)

    def ry(zd, h):
        part = ypart(h)
        return remote(
            pl_buf.at[zd * NY + (1 - y), *part], yr.at[zd, *part], sent.at[RY_S],
            ry_r.at[zd, h], col=yp,
        )

    def rh(f):
        part = zrows(f)
        return remote(pl_buf.at[yp, part], yr.at[z, part], sent.at[RH_S], rh_r.at[f], col=yp)

    def rz(zd, h, up):
        slot = zd + 1 if up else zd
        to = col + NY if up else col - NY
        part = ypart(h)
        return remote(
            pl_buf.at[zd * NY + y, *part], zr.at[slot, *part], sent.at[RZ_S],
            rz_r.at[slot, h], col=to,
        )

    def rf(zd, f, up):
        slot = zd + 1 if up else zd
        to = col + NY if up else col - NY
        part = zrows(f)
        return remote(
            pl_buf.at[zd * NY + y, part], zr.at[slot, part], sent.at[RZ_S],
            rf_r.at[slot, f], col=to,
        )

    def rq(zd, f, up):
        slot = zd + 1 if up else zd
        to = col + NY if up else col - NY
        return remote(
            pl_buf.at[zd * NY + (1 - y), zrows(f)], zq.at[slot, zrows(f, 0)], sent.at[RQ_S],
            rq_r.at[slot, f], col=to,
        )

    def held(k):
        return k // (kr * CORES) * kr + k % kr

    def pr_copy(k):
        slot = held(k)
        return remote(pu.at[k], pr.at[slot], sent.at[PR_S], pr_r.at[slot], row=partner)

    def pu_copy(k):
        return remote(pu.at[k], ur.at[x, k % kr], sent.at[PU_S], pu_r.at[x, k % kr], row=k // kr)

    def pu_got(x2, p):
        return remote(
            pu.at[0], ur.at[x2, p], sent.at[PU_S], pu_r.at[x2, p], row=x2 * CORES + core
        )

    def keeps(k):
        return (k // kr) % CORES == core

    def leaves(k):
        return k // (kr * CORES) != x

    def d_copy(r2, c):
        return remote(ds.at[c], dr.at[row, c], sent.at[D_S], d_r.at[row, c], row=r2)

    def d_got(r2, c):
        return remote(ds.at[c], dr.at[r2, c], sent.at[D_S], d_r.at[r2, c], row=r2)

    def d_relay(x2, c):
        r2 = x2 * CORES + core
        blk = dr.at[r2, c]
        return remote(blk, blk, sent.at[D_S], d_r.at[r2, c], row=partner)

    def each_dir(fn):
        @pl.when(z > 0)
        def _():
            fn(False)

        @pl.when(z < nz - 1)
        def _():
            fn(True)

    def row_member(k, i):
        m = mem[k, row * rs + i]
        return m >= 0, jnp.clip(m - row * rb, 0, rb - 1)

    def col_member(k, j):
        m = mem[k, col * cs + j]
        return m >= 0, jnp.clip(m - col * cb, 0, cb - 1)

    planes = nz // nx
    edge = jnp.logical_or(z == 0, z == nz - 1)

    def mine(zs):
        return zs // planes == x

    def last_to(up):
        e = nz - 1 if up else 0
        return jnp.where(mine(e), nz - 2 if up else 1, nz - 1 - e)

    def held_back(zs, up):
        return jnp.logical_and(z == (nz - 2 if up else 1), zs == last_to(up))

    def order(i):
        near_half = jnp.where(i % 2 == 0, nz // 2 + i // 2, i // 2)
        dist = jnp.where(mine(z), near_half, i)
        inner_low = jnp.where(i < nz // 2, nz // 2 + i, nz - 1 - i)
        inner_high = jnp.where(i < nz // 2, nz // 2 - 1 - i, i)
        return jnp.where(
            edge, jnp.where(z == 0, dist, nz - 1 - dist),
            jnp.where(2 * x < nx, inner_low, inner_high),
        )

    zero = jnp.zeros((), BF)

    def block(i):
        return pl.ds(pl.multiple_of(i * side, side), side)

    def lower_part(k):
        cols = [col_member(k, j) for j in range(cs)]
        panels = [jnp.where(cols[j][0], lbuf[k, j], zero) for j in range(cs)]

        def one(i, _):
            ok, ri = row_member(k, i)
            tot = None
            for j in range(cs):
                t = jnp.dot(a[ri, cols[j][1]], panels[j], preferred_element_type=F32)
                tot = t if tot is None else tot + t
            pl_buf[k, block(i)] = jnp.where(ok, tot, 0.0).astype(BF)
            return 0

        lax.fori_loop(0, rs, one, 0)

    def upper_part(k):
        mem_rows = [row_member(k, i) for i in range(rs)]

        def one(j, _):
            ok, cj = col_member(k, j)
            tot = None
            for i in range(rs):
                t = jnp.dot(
                    jnp.where(mem_rows[i][0], ubuf[k, block(i)], zero), a[mem_rows[i][1], cj],
                    preferred_element_type=F32,
                )
                tot = t if tot is None else tot + t
            pu[k, j] = jnp.where(ok, tot, 0.0).astype(BF)
            return 0

        lax.fori_loop(0, cs, one, 0)

        @pl.when(jnp.logical_not(keeps(k)))
        def _():
            pr_copy(k).start()

    def finish(k):
        @pl.when(jnp.logical_and(keeps(k), leaves(k)))
        def _():
            pr_copy(k).wait_recv()
            for j in range(cs):
                pu[k, j] = (pu[k, j].astype(F32) + pr[held(k), j].astype(F32)).astype(BF)
            pu_copy(k).start()

    def lower_group(r2):
        def one(p, _):
            k = r2 * kr + (p + 1 - y) % NY
            lower_part(k)

            @pl.when(k % NY != y)
            def _():
                for h in range(nyp):
                    ry(k // NY, h).start()

            return 0

        lax.fori_loop(0, kr, one, 0)

    def both_groups(x2):
        def one(q, _):
            lower_group(x2 * CORES + jnp.where(2 * x2 >= nx, CORES - 1 - q, q))
            return 0

        lax.fori_loop(0, CORES, one, 0)

    cu.wait()
    uy_own(0).start()
    each_dir(lambda up: uz(z, 0, up).start())
    each_dir(lambda up: uz(z, 1, up).start())
    cl.wait()
    l_own(partner).start()
    for dx in range(1, nx):
        l_own(((x + dx) % nx) * CORES + core).start()
    cm.wait()
    ca.wait()
    l_recv(partner).wait_recv()
    both_groups(x)

    uy_got(0, z).wait_recv()

    def share(zs, up):
        @pl.when(jnp.logical_not(held_back(zs, up)))
        def _():
            uz(zs, 2, up).start()

    each_dir(lambda up: share(z, up))
    upper_part(col)

    def others(fn):
        for dx in range(1, nx):
            fn((x + dx) % nx)

    def add_to(k, part, terms):
        tot = pl_buf[k, *part].astype(F32)
        for t in terms:
            tot = tot + t.astype(F32)
        pl_buf[k, *part] = tot.astype(BF)

    def each_way(zd, go):
        @pl.when(zd > z)
        def _():
            go(True)

        @pl.when(zd < z)
        def _():
            go(False)

    def hop_f(zd, f, own):
        k = zd * NY + (y if own else 1 - y)
        part = zrows(f)

        def go(up):
            slot = zd + 1 if up else zd
            step = (rf if own else rq)(zd, f, up)

            @pl.when((z > 0) if up else (z < nz - 1))
            def _():
                step.wait_recv()
                add_to(k, (part,), [zr[slot, part] if own else zq[slot, zrows(f, 0)]])

            step.start()

        each_way(zd, go)

    def hop_y(zd, h):
        k = zd * NY + y
        part = ypart(h)

        def go(up):
            slot = zd + 1 if up else zd
            step = rz(zd, h, up)
            ry(zd, h).wait_recv()

            @pl.when((z > 0) if up else (z < nz - 1))
            def _():
                step.wait_recv()
                add_to(k, part, [yr[zd, *part], zr[slot, *part]])

            @pl.when((z == 0) if up else (z == nz - 1))
            def _():
                add_to(k, part, [yr[zd, *part]])

            step.start()

        each_way(zd, go)

    def firsts(zds, own):
        def one(f, _):
            for zd, ok in zds:
                @pl.when(ok)
                def _():
                    hop_f(zd, f, own)

            return 0

        lax.fori_loop(0, nf, one, 0)

    def ends(j):
        return [(jnp.where(z == 0, nz - 1 - j, j), j < nz - 1)]

    def opening(early):
        def one(j, _):
            zd = ends(j)[0][0]
            firsts([(zd, mine(zd) if early else jnp.logical_not(mine(zd)))], False)
            return 0

        lax.fori_loop(0, nz - 1, one, 0)

    def relay(x2):
        l_recv(x2 * CORES + core).wait_recv()
        l_recv(x2 * CORES + core).start()

    def by_side(d, fn):
        @pl.when(z - d >= 0)
        def _():
            fn(z - d, True)

        @pl.when(z + d <= nz - 1)
        def _():
            fn(z + d, False)

    def take(kind):
        def one(zs, up):
            uz(zs, kind, up).wait_recv()

            @pl.when((z < nz - 1) if up else (z > 0))
            def _():
                if kind == 2:
                    share(zs, up)
                else:
                    uz(zs, kind, up).start()

        return one

    by_side(1, take(0))

    @pl.when(edge)
    def _():
        opening(True)

    others(relay)
    by_side(1, take(1))

    def late(x2):
        l_recv(x2 * CORES + 1 - core).wait_recv()
        both_groups(x2)

    others(late)

    @pl.when(edge)
    def _():
        opening(False)

    @pl.when(jnp.logical_not(edge))
    def _():
        by_side(1, take(2))

    def hand_on(zs):
        @pl.when(zs == z)
        def _():
            uy_own(1).start()

        @pl.when(zs != z)
        def _():
            uy_pass(zs).start()

    def sides(d, fn):
        def one(s, _):
            zs = z + (2 * s - 1) * d

            @pl.when(jnp.logical_and(zs >= 0, zs < nz))
            def _():
                fn(zs)

            return 0

        lax.fori_loop(0, 2, one, 0)

    def near(d):
        sides(d, lambda zs: upper_part(zs * NY + y))

    def near_done(d):
        sides(d, lambda zs: finish(zs * NY + y))

    def across(i):
        zs = order(i)

        @pl.when(jnp.logical_and(edge, zs > z))
        def _():
            uz(zs, 2, False).wait_recv()

        @pl.when(jnp.logical_and(edge, zs < z))
        def _():
            uz(zs, 2, True).wait_recv()

        uy_got(1, zs).wait_recv()
        upper_part(zs * NY + (1 - y))

    def across_done(i):
        finish(order(i) * NY + (1 - y))

    def home():
        def one(f, _):
            each_dir(lambda up: rq(z, f, not up).wait_recv())

            @pl.when(z > 0)
            def _():
                add_to(yp, (zrows(f),), [zq[z + 1, zrows(f, 0)]])

            @pl.when(z < nz - 1)
            def _():
                add_to(yp, (zrows(f),), [zq[z, zrows(f, 0)]])

            rh(f).start()
            return 0

        lax.fori_loop(0, nf, one, 0)

    def seconds(zds, hook=None, close=None):
        def piece(h, _):
            if hook is not None:
                hook(h)
            for zd, ok in zds:
                @pl.when(ok)
                def _():
                    hop_y(zd, h)

                if close is not None and zd is zds[0][0]:
                    @pl.when(h == nyp - 1)
                    def _():
                        close()

            return 0

        lax.fori_loop(0, nyp, piece, 0)

    near(1)
    finish(col)

    @pl.when(edge)
    def _():
        firsts(ends(0), True)
        seconds(ends(0))
        firsts(ends(1), True)

        def on(dist):
            hand_on(jnp.where(z == 0, dist, nz - 1 - dist))

        def one(d, _):
            by_side(d, take(0))

            @pl.when(jnp.logical_and(mine(z), d >= nz // 2))
            def _():
                on(d)

                @pl.when(d < nz - 1)
                def _():
                    on(d - nz // 2)

            @pl.when(jnp.logical_not(mine(z)))
            def _():
                @pl.when(d == 2)
                def _():
                    on(0)
                    on(1)

                @pl.when(d < nz - 1)
                def _():
                    on(d)

            by_side(d, take(1))
            near(d)
            near_done(d - 1)
            seconds(ends(d - 1))
            firsts(ends(d), True)
            return 0

        lax.fori_loop(2, nz, one, 0)
        across(0)
        near_done(nz - 1)
        home()
        hand_on(order(nz - 1))
        across(1)
        across_done(0)

    @pl.when(jnp.logical_not(edge))
    def _():
        low_half = 2 * z < nz
        short = jnp.where(low_half, z, nz - 1 - z)
        gap = nz - 1 - 2 * short
        spot = nyp - 2

        def both(s):
            s2 = s - gap
            return [
                (
                    jnp.where(low_half, s2, nz - 1 - s2),
                    jnp.logical_and(s2 >= 0, s2 < short),
                ),
                (jnp.where(low_half, nz - 1 - s, s), s >= 0),
            ]

        def others_long(s, _):
            firsts(both(s)[1:], False)
            return 0

        def others_short(s, _):
            firsts(both(s)[:1], False)
            return 0

        def one(d, _):
            by_side(d, take(0))
            by_side(d, take(1))

            @pl.when(d == nz - 2)
            def _():
                lax.fori_loop(0, nz - 1 - short, others_long, 0)

            by_side(d, take(2))
            near(d)
            near_done(d - 1)
            return 0

        lax.fori_loop(2, nz - 1, one, 0)
        for i in range(nz - 1):
            hand_on(order(i))
        def pair(s, _):
            s2 = s - gap

            def hook(h):
                now = s == nz - 2 - short

                @pl.when(jnp.logical_and(now, h - spot == 0))
                def _():
                    near_done(nz - 2)
                    across(0)

                @pl.when(jnp.logical_and(now, h - spot == 1))
                def _():
                    across(1)

            def close():
                @pl.when(s2 == short - 1)
                def _():
                    @pl.when(z == 1)
                    def _():
                        uz(last_to(False), 2, False).start()

                    @pl.when(z == nz - 2)
                    def _():
                        uz(last_to(True), 2, True).start()

            firsts(both(s), True)

            @pl.when(s == 0)
            def _():
                lax.fori_loop(0, nz - 1 - short, others_short, 0)

            seconds(both(s), hook, close)

            @pl.when(s == 0)
            def _():
                home()
                hand_on(order(nz - 1))

            return 0

        lax.fori_loop(0, nz - 1 - short, pair, 0)
        across_done(0)

    across_done(1)

    def rest(i, _):
        across(i)

        @pl.when(i > 2)
        def _():
            across_done(i - 1)

        return 0

    lax.fori_loop(2, nz - 1, rest, 0)

    def final(part, got, step):
        got.wait_recv()
        acc[*part] = pl_buf[col, *part].astype(F32) + yr[z, *part].astype(F32)

        @pl.when(z > 0)
        def _():
            step(True).wait_recv()
            acc[*part] = acc[*part] + zr[z + 1, *part].astype(F32)

        @pl.when(z < nz - 1)
        def _():
            step(False).wait_recv()
            acc[*part] = acc[*part] + zr[z, *part].astype(F32)

        low_out[0, *part] = (-acc[*part]).astype(BF)

    def final_f(f, _):
        final((zrows(f),), rh(f), lambda up: rf(z, f, up))
        return 0

    def final_y(h, _):
        final(ypart(h), ry(z, h), lambda up: rz(z, h, up))
        return 0

    lax.fori_loop(0, nf, final_f, 0)

    def side_sum(c, _):
        lax.fori_loop(c * nh, (c + 1) * nh, final_y, 0)
        cols = pl.ds(pl.multiple_of(c * half, half), half)
        tot = None
        for i in range(rs):
            t = jnp.dot(
                jnp.where(row_member(col, i)[0], ubuf[col, block(i)], zero),
                low_out[0, block(i), cols],
                preferred_element_type=F32,
            )
            tot = t if tot is None else tot + t
        dacc[c] = tot
        ds[c] = tot.astype(BF)
        others(lambda x2: d_copy(x2 * CORES + core, c).start())
        d_copy(partner, c).start()
        return 0

    lax.fori_loop(0, 2, side_sum, 0)

    across_done(nz - 2)

    def d_pass(x2):
        for c in range(2):
            d_got(x2 * CORES + core, c).wait_recv()
            d_relay(x2, c).start()

    @pl.when(edge)
    def _():
        others(d_pass)

    across(nz - 1)
    across_done(nz - 1)

    @pl.when(jnp.logical_not(edge))
    def _():
        others(d_pass)

    def piece(p, j):
        return block(p * cs + j)

    for p in range(kr):
        pr_copy(row * kr + p).wait_recv()
        for j in range(cs):
            acc[piece(p, j)] = (
                pu[row * kr + p, j].astype(F32) + pr[held(row * kr + p), j].astype(F32)
            )

    def pu_add(x2):
        for p in range(kr):
            pu_got(x2, p).wait_recv()
            for j in range(cs):
                acc[piece(p, j)] = acc[piece(p, j)] + ur[x2, p, j].astype(F32)

    others(pu_add)
    for p in range(kr):
        for j in range(cs):
            upp_out[p, j] = (-acc[piece(p, j)]).astype(BF)

    def all_sent(ref, which):
        pltpu.make_async_copy(ref, ref, sent.at[which]).wait()

    for kind in range(3):
        n = nq if kind else ny

        @pl.when(edge)
        def _():
            all_sent(ubuf.at[pl.ds(0, 1), pl.ds(0, n)], UZ_S + kind)

        @pl.when(jnp.logical_not(edge))
        def _():
            all_sent(ubuf.at[pl.ds(0, nz + 1), pl.ds(0, n)], UZ_S + kind)

    all_sent(lbuf.at[pl.ds(0, kr * (2 * nx - 1))], L_S)
    all_sent(ubuf.at[pl.ds(0, 1), pl.ds(0, nq)], UA_S)
    all_sent(ubuf.at[pl.ds(0, nz), pl.ds(0, ny)], UY_S)
    all_sent(pl_buf.at[pl.ds(0, nz), pl.ds(0, yf)], RY_S)
    all_sent(pl_buf.at[pl.ds(0, 1), pl.ds(0, nf * pz)], RH_S)
    all_sent(pl_buf.at[pl.ds(0, nz - 1)], RZ_S)
    all_sent(pl_buf.at[pl.ds(0, nz - 1), pl.ds(0, nf * pz)], RQ_S)
    all_sent(pu.at[pl.ds(0, n_col // CORES)], PR_S)
    all_sent(pu.at[pl.ds(0, kr * (nx - 1))], PU_S)

    cp.wait()

    def d_sum(c, _):
        def d_add(r2):
            dacc[c] = dacc[c] + dr[r2, c].astype(F32)

        d_got(partner, c).wait_recv()
        d_add(partner)

        def d_add_chip(x2):
            d_add(x2 * CORES + core)
            d_got(x2 * CORES + 1 - core, c).wait_recv()
            d_add(x2 * CORES + 1 - core)

        others(d_add_chip)
        cols = pl.ds(pl.multiple_of(c * half, half), half)
        diag_out[0, :, cols] = piv[:, cols] - dacc[c]
        return 0

    lax.fori_loop(0, 2, d_sum, 0)
    all_sent(dr.at[pl.ds(0, 2 * nx - 1)], D_S)


def hand_over(low, upp, diag, low_to, upp_to, diag_to, sems):
    side = diag.shape[1]
    pairs = [(upp, upp_to), (diag, diag_to)]
    for h in range(low_to.shape[1]):
        pairs.append((low.at[0, pl.ds(h * side, side)], low_to.at[0, h]))
    copies = [pltpu.make_async_copy(a, b, sems.at[i]) for i, (a, b) in enumerate(pairs)]
    for c in copies:
        c.start()
    for c in copies:
        c.wait()


def body(ancestor_inv, lower_panel, upper_panel, pivot_inv, members):
    n_col = lax.axis_size("col")
    n_row = lax.axis_size("row")
    side = ancestor_inv.shape[2]
    rb, cb = ancestor_inv.shape[:2]
    kr, cs = lower_panel.shape[:2]
    per_col, rs = upper_panel.shape[:2]
    level = members.shape[0]
    nz = n_col // NY
    assert per_col == 1 and level == n_col and kr == NY and nz == n_row
    rows = rs * side
    nf, nyp = 1, 2
    pz = rows * 3 // 8
    py = (rows - nf * pz) // nyp
    nq = rows * 25 // 64
    assert nf * pz + nyp * py == rows and pz % 16 == 0 and py % 16 == 0 and nq % 16 == 0
    blk = (side, side)
    dma = pltpu.SemaphoreType.DMA
    vmem = pl.BlockSpec(memory_space=pltpu.VMEM)
    hbm = pl.BlockSpec(memory_space=pltpu.HBM)
    outs = pl.pallas_call(
        functools.partial(kernel, n_row, n_col, nq, nf, pz, nyp, py),
        out_shape=(
            pltpu.VMEM((per_col, rows, side), BF),
            pltpu.VMEM((kr, cs) + blk, BF),
            pltpu.VMEM((per_col,) + blk, F32),
        ),
        in_specs=[hbm] * 5,
        out_specs=(vmem, vmem, vmem),
        scratch_shapes=[
            pltpu.SMEM(members.shape, jnp.int32),
            pltpu.VMEM(blk, F32),
            pltpu.VMEM((rb, cb) + blk, BF),
            pltpu.VMEM((level, cs) + blk, BF),
            pltpu.VMEM((n_col, rows, side), BF),
            pltpu.VMEM((n_col, rows, side), BF),
            pltpu.VMEM((nz, rows, side), BF),
            pltpu.VMEM((nz + 1, rows, side), BF),
            pltpu.VMEM((nz + 1, nf * pz, side), BF),
            pltpu.VMEM((level, cs) + blk, BF),
            pltpu.VMEM((level // CORES, cs) + blk, BF),
            pltpu.VMEM((n_row // CORES, kr, cs) + blk, BF),
            pltpu.VMEM((2, side, side // 2), BF),
            pltpu.VMEM((n_row, 2, side, side // 2), BF),
            pltpu.VMEM((max(rs, kr * cs) * side, side), F32),
            pltpu.VMEM((2, side, side // 2), F32),
            dma((5,)), dma((13,)), dma((n_row,)), dma((nz + 1,)), dma((nz, 3)),
            dma((nz, nyp)), dma((nf,)), dma((nz + 1, nyp)), dma((nz + 1, nf)),
            dma((nz + 1, nf)), dma((n_col // CORES,)), dma((n_row // CORES, kr)), dma((n_row, 2)),
        ],
        compiler_params=pltpu.CompilerParams(
            collective_id=0, has_side_effects=True, vmem_limit_bytes=60 * 1024 * 1024
        ),
    )(members, ancestor_inv, lower_panel, upper_panel.reshape(per_col, rows, side), pivot_inv)
    return pl.pallas_call(
        hand_over,
        out_shape=(
            jax.ShapeDtypeStruct((per_col, rs) + blk, BF),
            jax.ShapeDtypeStruct((kr, cs) + blk, BF),
            jax.ShapeDtypeStruct((per_col,) + blk, F32),
        ),
        in_specs=[vmem] * 3,
        out_specs=(hbm,) * 3,
        scratch_shapes=[dma((rs + 2,))],
    )(*(pltpu.with_memory_space_constraint(o, pltpu.VMEM) for o in outs))


def solution(mesh):
    return jax.shard_map(
        body,
        mesh=mesh,
        in_specs=(
            P("row", "col", None, None),
            P("row", "col", None, None),
            P("col", "row", None, None),
            P("col", None, None),
            P(),
        ),
        out_specs=(P("col", "row", None, None), P("row", "col", None, None), P("col", None, None)),
        check_vma=False,
    )
```

```python
import functools

import jax
import jax.numpy as jnp
from jax import lax
from jax.experimental import pallas as pl
from jax.experimental.pallas import tpu as pltpu
from jax.sharding import PartitionSpec as P

NY = 2
CORES = 2
BF = jnp.bfloat16
F32 = jnp.float32


def kernel(
    n_row, n_col, nq, nf, pz, nyp, py,
    mem_in, anc, low, upp, piv_in,
    low_out, upp_out, diag_out,
    mem, piv, a, lbuf, ubuf, pl_buf, yr, zr, zq, pu, pr, ur, ds, dr, acc, dacc,
    loc, sent, l_r, uy_r, uz_r, ry_r, rh_r, rz_r, rf_r, rq_r,
    pr_r, pu_r, d_r,
):
    row = lax.axis_index("row")
    col = lax.axis_index("col")
    nz = n_col // NY
    nx = n_row // CORES
    x, core = row // CORES, row % CORES
    z, y = col // NY, col % NY
    yp = z * NY + (1 - y)
    rb, cb = anc.shape[0], anc.shape[1]
    kr, cs = low.shape[0], low.shape[1]
    side = low.shape[2]
    rows = upp.shape[1]
    rs = rows // side
    ny = rows - nq
    yf = nyp * py
    partner = x * CORES + (1 - core)

    def remote(src, dst, ss, rsem, **where):
        return pltpu.make_async_remote_copy(
            src_ref=src, dst_ref=dst, send_sem=ss, recv_sem=rsem, device_id=where
        )

    ca = pltpu.make_async_copy(anc, a, loc.at[0])
    cl = pltpu.make_async_copy(low, lbuf.at[pl.ds(row * kr, kr)], loc.at[1])
    cu = pltpu.make_async_copy(upp.at[0], ubuf.at[col], loc.at[2])
    cp = pltpu.make_async_copy(piv_in.at[0], piv, loc.at[3])
    cm = pltpu.make_async_copy(mem_in, mem, loc.at[4])

    bar = pltpu.get_barrier_semaphore()
    for dx in range(1, n_row):
        pl.semaphore_signal(bar, inc=1, device_id={"row": (row + dx) % n_row})
    pl.semaphore_signal(bar, inc=1, device_id={"col": yp})

    @pl.when(z > 0)
    def _():
        pl.semaphore_signal(bar, inc=1, device_id={"col": col - NY})

    @pl.when(z < nz - 1)
    def _():
        pl.semaphore_signal(bar, inc=1, device_id={"col": col + NY})

    cu.start()
    cl.start()
    ca.start()
    cm.start()
    cp.start()
    peers = n_row + jnp.where(z > 0, 1, 0) + jnp.where(z < nz - 1, 1, 0)
    pl.semaphore_wait(bar, peers)

    L_S, UA_S, UY_S, RY_S, RH_S, RZ_S, RQ_S, PR_S, PU_S, D_S, UZ_S = range(11)

    def l_own(r2):
        blk = lbuf.at[pl.ds(row * kr, kr)]
        return remote(blk, blk, sent.at[L_S], l_r.at[row], row=r2)

    def l_recv(r2):
        blk = lbuf.at[pl.ds(r2 * kr, kr)]
        return remote(blk, blk, sent.at[L_S], l_r.at[r2], row=partner)

    def uy(k, late, rsem):
        part = pl.ds(0, ny) if late else pl.ds(ny, nq)
        blk = ubuf.at[k, part]
        return remote(blk, blk, sent.at[UY_S if late else UA_S], uy_r.at[rsem], col=yp)

    def uy_own(kind):
        return uy(col, kind == 1, z if kind else nz)

    def uy_got(kind, zs):
        return uy(zs * NY + (1 - y), kind == 1, zs if kind else nz)

    def uy_pass(zs):
        return uy(zs * NY + y, True, zs)

    def uz(zs, kind, up):
        k = zs * NY + (1 - y if kind == 2 else y)
        blk = ubuf.at[k, pl.ds(0, ny) if kind == 0 else pl.ds(ny, nq)]
        to = col + NY if up else col - NY
        return remote(blk, blk, sent.at[UZ_S + kind], uz_r.at[zs, kind], col=to)

    half = side // 2
    nh = nyp // 2

    def ypart(h):
        return (
            pl.ds(pl.multiple_of((h % nh) * (2 * py), 16), 2 * py),
            pl.ds(pl.multiple_of((h // nh) * half, half), half),
        )

    def zrows(f, base=yf):
        return pl.ds(pl.multiple_of(base + f * pz, 16), pz)

    def ry(zd, h):
        part = ypart(h)
        return remote(
            pl_buf.at[zd * NY + (1 - y), *part], yr.at[zd, *part], sent.at[RY_S],
            ry_r.at[zd, h], col=yp,
        )

    def rh(f):
        part = zrows(f)
        return remote(pl_buf.at[yp, part], yr.at[z, part], sent.at[RH_S], rh_r.at[f], col=yp)

    def rz(zd, h, up):
        slot = zd + 1 if up else zd
        to = col + NY if up else col - NY
        part = ypart(h)
        return remote(
            pl_buf.at[zd * NY + y, *part], zr.at[slot, *part], sent.at[RZ_S],
            rz_r.at[slot, h], col=to,
        )

    def rf(zd, f, up):
        slot = zd + 1 if up else zd
        to = col + NY if up else col - NY
        part = zrows(f)
        return remote(
            pl_buf.at[zd * NY + y, part], zr.at[slot, part], sent.at[RZ_S],
            rf_r.at[slot, f], col=to,
        )

    def rq(zd, f, up):
        slot = zd + 1 if up else zd
        to = col + NY if up else col - NY
        return remote(
            pl_buf.at[zd * NY + (1 - y), zrows(f)], zq.at[slot, zrows(f, 0)], sent.at[RQ_S],
            rq_r.at[slot, f], col=to,
        )

    def held(k):
        return k // (kr * CORES) * kr + k % kr

    def pr_copy(k):
        slot = held(k)
        return remote(pu.at[k], pr.at[slot], sent.at[PR_S], pr_r.at[slot], row=partner)

    def pu_copy(k):
        return remote(pu.at[k], ur.at[x, k % kr], sent.at[PU_S], pu_r.at[x, k % kr], row=k // kr)

    def pu_got(x2, p):
        return remote(
            pu.at[0], ur.at[x2, p], sent.at[PU_S], pu_r.at[x2, p], row=x2 * CORES + core
        )

    def keeps(k):
        return (k // kr) % CORES == core

    def leaves(k):
        return k // (kr * CORES) != x

    def d_copy(r2, c):
        return remote(ds.at[c], dr.at[row, c], sent.at[D_S], d_r.at[row, c], row=r2)

    def d_got(r2, c):
        return remote(ds.at[c], dr.at[r2, c], sent.at[D_S], d_r.at[r2, c], row=r2)

    def d_relay(x2, c):
        r2 = x2 * CORES + core
        blk = dr.at[r2, c]
        return remote(blk, blk, sent.at[D_S], d_r.at[r2, c], row=partner)

    def each_dir(fn):
        @pl.when(z > 0)
        def _():
            fn(False)

        @pl.when(z < nz - 1)
        def _():
            fn(True)

    def row_member(k, i):
        m = mem[k, row * rs + i]
        return m >= 0, jnp.clip(m - row * rb, 0, rb - 1)

    def col_member(k, j):
        m = mem[k, col * cs + j]
        return m >= 0, jnp.clip(m - col * cb, 0, cb - 1)

    planes = nz // nx
    edge = jnp.logical_or(z == 0, z == nz - 1)

    def mine(zs):
        return zs // planes == x

    def last_to(up):
        e = nz - 1 if up else 0
        return jnp.where(mine(e), nz - 2 if up else 1, nz - 1 - e)

    def held_back(zs, up):
        return jnp.logical_and(z == (nz - 2 if up else 1), zs == last_to(up))

    def order(i):
        near_half = jnp.where(i % 2 == 0, nz // 2 + i // 2, i // 2)
        dist = jnp.where(mine(z), near_half, i)
        inner_low = jnp.where(i < nz // 2, nz // 2 + i, nz - 1 - i)
        inner_high = jnp.where(i < nz // 2, nz // 2 - 1 - i, i)
        return jnp.where(
            edge, jnp.where(z == 0, dist, nz - 1 - dist),
            jnp.where(2 * x < nx, inner_low, inner_high),
        )

    zero = jnp.zeros((), BF)

    def block(i):
        return pl.ds(pl.multiple_of(i * side, side), side)

    def lower_part(k):
        cols = [col_member(k, j) for j in range(cs)]
        panels = [jnp.where(cols[j][0], lbuf[k, j], zero) for j in range(cs)]

        def one(i, _):
            ok, ri = row_member(k, i)
            tot = None
            for j in range(cs):
                t = jnp.dot(a[ri, cols[j][1]], panels[j], preferred_element_type=F32)
                tot = t if tot is None else tot + t
            pl_buf[k, block(i)] = jnp.where(ok, tot, 0.0).astype(BF)
            return 0

        lax.fori_loop(0, rs, one, 0)

    def upper_part(k):
        mem_rows = [row_member(k, i) for i in range(rs)]

        def one(j, _):
            ok, cj = col_member(k, j)
            tot = None
            for i in range(rs):
                t = jnp.dot(
                    jnp.where(mem_rows[i][0], ubuf[k, block(i)], zero), a[mem_rows[i][1], cj],
                    preferred_element_type=F32,
                )
                tot = t if tot is None else tot + t
            pu[k, j] = jnp.where(ok, tot, 0.0).astype(BF)
            return 0

        lax.fori_loop(0, cs, one, 0)

        @pl.when(jnp.logical_not(keeps(k)))
        def _():
            pr_copy(k).start()

    def finish(k):
        @pl.when(jnp.logical_and(keeps(k), leaves(k)))
        def _():
            pr_copy(k).wait_recv()
            for j in range(cs):
                pu[k, j] = (pu[k, j].astype(F32) + pr[held(k), j].astype(F32)).astype(BF)
            pu_copy(k).start()

    def lower_group(r2):
        def one(p, _):
            k = r2 * kr + (p + 1 - y) % NY
            lower_part(k)

            @pl.when(k % NY != y)
            def _():
                for h in range(nyp):
                    ry(k // NY, h).start()

            return 0

        lax.fori_loop(0, kr, one, 0)

    def both_groups(x2):
        def one(q, _):
            lower_group(x2 * CORES + jnp.where(2 * x2 >= nx, CORES - 1 - q, q))
            return 0

        lax.fori_loop(0, CORES, one, 0)

    cu.wait()
    uy_own(0).start()
    each_dir(lambda up: uz(z, 0, up).start())
    each_dir(lambda up: uz(z, 1, up).start())
    cl.wait()
    l_own(partner).start()
    for dx in range(1, nx):
        l_own(((x + dx) % nx) * CORES + core).start()
    cm.wait()
    ca.wait()
    l_recv(partner).wait_recv()
    both_groups(x)

    uy_got(0, z).wait_recv()

    def share(zs, up):
        @pl.when(jnp.logical_not(held_back(zs, up)))
        def _():
            uz(zs, 2, up).start()

    each_dir(lambda up: share(z, up))
    upper_part(col)

    def others(fn):
        for dx in range(1, nx):
            fn((x + dx) % nx)

    def add_to(k, part, terms):
        tot = pl_buf[k, *part].astype(F32)
        for t in terms:
            tot = tot + t.astype(F32)
        pl_buf[k, *part] = tot.astype(BF)

    def each_way(zd, go):
        @pl.when(zd > z)
        def _():
            go(True)

        @pl.when(zd < z)
        def _():
            go(False)

    def hop_f(zd, f, own):
        k = zd * NY + (y if own else 1 - y)
        part = zrows(f)

        def go(up):
            slot = zd + 1 if up else zd
            step = (rf if own else rq)(zd, f, up)

            @pl.when((z > 0) if up else (z < nz - 1))
            def _():
                step.wait_recv()
                add_to(k, (part,), [zr[slot, part] if own else zq[slot, zrows(f, 0)]])

            step.start()

        each_way(zd, go)

    def hop_y(zd, h):
        k = zd * NY + y
        part = ypart(h)

        def go(up):
            slot = zd + 1 if up else zd
            step = rz(zd, h, up)
            ry(zd, h).wait_recv()

            @pl.when((z > 0) if up else (z < nz - 1))
            def _():
                step.wait_recv()
                add_to(k, part, [yr[zd, *part], zr[slot, *part]])

            @pl.when((z == 0) if up else (z == nz - 1))
            def _():
                add_to(k, part, [yr[zd, *part]])

            step.start()

        each_way(zd, go)

    def firsts(zds, own):
        def one(f, _):
            for zd, ok in zds:
                @pl.when(ok)
                def _():
                    hop_f(zd, f, own)

            return 0

        lax.fori_loop(0, nf, one, 0)

    def ends(j):
        return [(jnp.where(z == 0, nz - 1 - j, j), j < nz - 1)]

    def opening(early):
        def one(j, _):
            zd = ends(j)[0][0]
            firsts([(zd, mine(zd) if early else jnp.logical_not(mine(zd)))], False)
            return 0

        lax.fori_loop(0, nz - 1, one, 0)

    def relay(x2):
        l_recv(x2 * CORES + core).wait_recv()
        l_recv(x2 * CORES + core).start()

    def by_side(d, fn):
        @pl.when(z - d >= 0)
        def _():
            fn(z - d, True)

        @pl.when(z + d <= nz - 1)
        def _():
            fn(z + d, False)

    def take(kind):
        def one(zs, up):
            uz(zs, kind, up).wait_recv()

            @pl.when((z < nz - 1) if up else (z > 0))
            def _():
                if kind == 2:
                    share(zs, up)
                else:
                    uz(zs, kind, up).start()

        return one

    by_side(1, take(0))

    @pl.when(edge)
    def _():
        opening(True)

    others(relay)
    by_side(1, take(1))

    def late(x2):
        l_recv(x2 * CORES + 1 - core).wait_recv()
        both_groups(x2)

    others(late)

    @pl.when(edge)
    def _():
        opening(False)

    @pl.when(jnp.logical_not(edge))
    def _():
        by_side(1, take(2))

    def hand_on(zs):
        @pl.when(zs == z)
        def _():
            uy_own(1).start()

        @pl.when(zs != z)
        def _():
            uy_pass(zs).start()

    def sides(d, fn):
        def one(s, _):
            zs = z + (2 * s - 1) * d

            @pl.when(jnp.logical_and(zs >= 0, zs < nz))
            def _():
                fn(zs)

            return 0

        lax.fori_loop(0, 2, one, 0)

    def near(d):
        sides(d, lambda zs: upper_part(zs * NY + y))

    def near_done(d):
        sides(d, lambda zs: finish(zs * NY + y))

    def across(i):
        zs = order(i)

        @pl.when(jnp.logical_and(edge, zs > z))
        def _():
            uz(zs, 2, False).wait_recv()

        @pl.when(jnp.logical_and(edge, zs < z))
        def _():
            uz(zs, 2, True).wait_recv()

        uy_got(1, zs).wait_recv()
        upper_part(zs * NY + (1 - y))

    def across_done(i):
        finish(order(i) * NY + (1 - y))

    def home():
        def one(f, _):
            each_dir(lambda up: rq(z, f, not up).wait_recv())

            @pl.when(z > 0)
            def _():
                add_to(yp, (zrows(f),), [zq[z + 1, zrows(f, 0)]])

            @pl.when(z < nz - 1)
            def _():
                add_to(yp, (zrows(f),), [zq[z, zrows(f, 0)]])

            rh(f).start()
            return 0

        lax.fori_loop(0, nf, one, 0)

    def seconds(zds, hook=None, close=None):
        def piece(h, _):
            if hook is not None:
                hook(h)
            for zd, ok in zds:
                @pl.when(ok)
                def _():
                    hop_y(zd, h)

                if close is not None and zd is zds[0][0]:
                    @pl.when(h == nyp - 1)
                    def _():
                        close()

            return 0

        lax.fori_loop(0, nyp, piece, 0)

    near(1)
    finish(col)

    @pl.when(edge)
    def _():
        firsts(ends(0), True)
        seconds(ends(0))
        firsts(ends(1), True)

        def on(dist):
            hand_on(jnp.where(z == 0, dist, nz - 1 - dist))

        def one(d, _):
            by_side(d, take(0))

            @pl.when(jnp.logical_and(mine(z), d >= nz // 2))
            def _():
                on(d)

                @pl.when(d < nz - 1)
                def _():
                    on(d - nz // 2)

            @pl.when(jnp.logical_not(mine(z)))
            def _():
                @pl.when(d == 2)
                def _():
                    on(0)
                    on(1)

                @pl.when(d < nz - 1)
                def _():
                    on(d)

            by_side(d, take(1))
            near(d)
            near_done(d - 1)
            seconds(ends(d - 1))
            firsts(ends(d), True)
            return 0

        lax.fori_loop(2, nz, one, 0)
        across(0)
        near_done(nz - 1)
        home()
        hand_on(order(nz - 1))
        across(1)
        across_done(0)

    @pl.when(jnp.logical_not(edge))
    def _():
        low_half = 2 * z < nz
        short = jnp.where(low_half, z, nz - 1 - z)
        gap = nz - 1 - 2 * short
        spot = nyp - 2

        def both(s):
            s2 = s - gap
            return [
                (
                    jnp.where(low_half, s2, nz - 1 - s2),
                    jnp.logical_and(s2 >= 0, s2 < short),
                ),
                (jnp.where(low_half, nz - 1 - s, s), s >= 0),
            ]

        def others_long(s, _):
            firsts(both(s)[1:], False)
            return 0

        def others_short(s, _):
            firsts(both(s)[:1], False)
            return 0

        def one(d, _):
            by_side(d, take(0))

            @pl.when(d == nz - 2)
            def _():
                for i in range(nz - 1):
                    hand_on(order(i))

            by_side(d, take(1))

            @pl.when(d == nz - 2)
            def _():
                lax.fori_loop(0, nz - 1 - short, others_long, 0)

            by_side(d, take(2))
            near(d)
            near_done(d - 1)
            return 0

        lax.fori_loop(2, nz - 1, one, 0)
        def pair(s, _):
            s2 = s - gap

            def hook(h):
                now = s == nz - 2 - short

                @pl.when(jnp.logical_and(now, h - spot == 0))
                def _():
                    near_done(nz - 2)
                    across(0)

                @pl.when(jnp.logical_and(now, h - spot == 1))
                def _():
                    across(1)

            def close():
                @pl.when(s2 == short - 1)
                def _():
                    @pl.when(z == 1)
                    def _():
                        uz(last_to(False), 2, False).start()

                    @pl.when(z == nz - 2)
                    def _():
                        uz(last_to(True), 2, True).start()

            firsts(both(s), True)

            @pl.when(s == 0)
            def _():
                lax.fori_loop(0, nz - 1 - short, others_short, 0)

            seconds(both(s), hook, close)

            @pl.when(s == 0)
            def _():
                home()
                hand_on(order(nz - 1))

            return 0

        lax.fori_loop(0, nz - 1 - short, pair, 0)
        across_done(0)

    across_done(1)

    def rest(i, _):
        across(i)

        @pl.when(i > 2)
        def _():
            across_done(i - 1)

        return 0

    lax.fori_loop(2, nz - 1, rest, 0)

    def final(part, got, step):
        got.wait_recv()
        acc[*part] = pl_buf[col, *part].astype(F32) + yr[z, *part].astype(F32)

        @pl.when(z > 0)
        def _():
            step(True).wait_recv()
            acc[*part] = acc[*part] + zr[z + 1, *part].astype(F32)

        @pl.when(z < nz - 1)
        def _():
            step(False).wait_recv()
            acc[*part] = acc[*part] + zr[z, *part].astype(F32)

        low_out[0, *part] = (-acc[*part]).astype(BF)

    def final_f(f, _):
        final((zrows(f),), rh(f), lambda up: rf(z, f, up))
        return 0

    def final_y(h, _):
        final(ypart(h), ry(z, h), lambda up: rz(z, h, up))
        return 0

    lax.fori_loop(0, nf, final_f, 0)

    def side_sum(c, _):
        lax.fori_loop(c * nh, (c + 1) * nh, final_y, 0)
        cols = pl.ds(pl.multiple_of(c * half, half), half)
        tot = None
        for i in range(rs):
            t = jnp.dot(
                jnp.where(row_member(col, i)[0], ubuf[col, block(i)], zero),
                low_out[0, block(i), cols],
                preferred_element_type=F32,
            )
            tot = t if tot is None else tot + t
        dacc[c] = tot
        ds[c] = tot.astype(BF)
        others(lambda x2: d_copy(x2 * CORES + core, c).start())
        d_copy(partner, c).start()
        return 0

    lax.fori_loop(0, 2, side_sum, 0)

    across_done(nz - 2)

    def d_pass(x2):
        for c in range(2):
            d_got(x2 * CORES + core, c).wait_recv()
            d_relay(x2, c).start()

    @pl.when(edge)
    def _():
        others(d_pass)

    across(nz - 1)
    across_done(nz - 1)

    @pl.when(jnp.logical_not(edge))
    def _():
        others(d_pass)

    def piece(p, j):
        return block(p * cs + j)

    for p in range(kr):
        pr_copy(row * kr + p).wait_recv()
        for j in range(cs):
            acc[piece(p, j)] = (
                pu[row * kr + p, j].astype(F32) + pr[held(row * kr + p), j].astype(F32)
            )

    def pu_add(x2):
        for p in range(kr):
            pu_got(x2, p).wait_recv()
            for j in range(cs):
                acc[piece(p, j)] = acc[piece(p, j)] + ur[x2, p, j].astype(F32)

    others(pu_add)
    for p in range(kr):
        for j in range(cs):
            upp_out[p, j] = (-acc[piece(p, j)]).astype(BF)

    def all_sent(ref, which):
        pltpu.make_async_copy(ref, ref, sent.at[which]).wait()

    for kind in range(3):
        n = nq if kind else ny

        @pl.when(edge)
        def _():
            all_sent(ubuf.at[pl.ds(0, 1), pl.ds(0, n)], UZ_S + kind)

        @pl.when(jnp.logical_not(edge))
        def _():
            all_sent(ubuf.at[pl.ds(0, nz + 1), pl.ds(0, n)], UZ_S + kind)

    all_sent(lbuf.at[pl.ds(0, kr * (2 * nx - 1))], L_S)
    all_sent(ubuf.at[pl.ds(0, 1), pl.ds(0, nq)], UA_S)
    all_sent(ubuf.at[pl.ds(0, nz), pl.ds(0, ny)], UY_S)
    all_sent(pl_buf.at[pl.ds(0, nz), pl.ds(0, yf)], RY_S)
    all_sent(pl_buf.at[pl.ds(0, 1), pl.ds(0, nf * pz)], RH_S)
    all_sent(pl_buf.at[pl.ds(0, nz - 1)], RZ_S)
    all_sent(pl_buf.at[pl.ds(0, nz - 1), pl.ds(0, nf * pz)], RQ_S)
    all_sent(pu.at[pl.ds(0, n_col // CORES)], PR_S)
    all_sent(pu.at[pl.ds(0, kr * (nx - 1))], PU_S)

    cp.wait()

    def d_sum(c, _):
        def d_add(r2):
            dacc[c] = dacc[c] + dr[r2, c].astype(F32)

        d_got(partner, c).wait_recv()
        d_add(partner)

        def d_add_chip(x2):
            d_add(x2 * CORES + core)
            d_got(x2 * CORES + 1 - core, c).wait_recv()
            d_add(x2 * CORES + 1 - core)

        others(d_add_chip)
        cols = pl.ds(pl.multiple_of(c * half, half), half)
        diag_out[0, :, cols] = piv[:, cols] - dacc[c]
        return 0

    lax.fori_loop(0, 2, d_sum, 0)
    all_sent(dr.at[pl.ds(0, 2 * nx - 1)], D_S)


def hand_over(low, upp, diag, low_to, upp_to, diag_to, sems):
    side = diag.shape[1]
    pairs = [(upp, upp_to), (diag, diag_to)]
    for h in range(low_to.shape[1]):
        pairs.append((low.at[0, pl.ds(h * side, side)], low_to.at[0, h]))
    copies = [pltpu.make_async_copy(a, b, sems.at[i]) for i, (a, b) in enumerate(pairs)]
    for c in copies:
        c.start()
    for c in copies:
        c.wait()


def body(ancestor_inv, lower_panel, upper_panel, pivot_inv, members):
    n_col = lax.axis_size("col")
    n_row = lax.axis_size("row")
    side = ancestor_inv.shape[2]
    rb, cb = ancestor_inv.shape[:2]
    kr, cs = lower_panel.shape[:2]
    per_col, rs = upper_panel.shape[:2]
    level = members.shape[0]
    nz = n_col // NY
    assert per_col == 1 and level == n_col and kr == NY and nz == n_row
    rows = rs * side
    nf, nyp = 1, 2
    pz = rows * 3 // 8
    py = (rows - nf * pz) // nyp
    nq = rows * 25 // 64
    assert nf * pz + nyp * py == rows and pz % 16 == 0 and py % 16 == 0 and nq % 16 == 0
    blk = (side, side)
    dma = pltpu.SemaphoreType.DMA
    vmem = pl.BlockSpec(memory_space=pltpu.VMEM)
    hbm = pl.BlockSpec(memory_space=pltpu.HBM)
    outs = pl.pallas_call(
        functools.partial(kernel, n_row, n_col, nq, nf, pz, nyp, py),
        out_shape=(
            pltpu.VMEM((per_col, rows, side), BF),
            pltpu.VMEM((kr, cs) + blk, BF),
            pltpu.VMEM((per_col,) + blk, F32),
        ),
        in_specs=[hbm] * 5,
        out_specs=(vmem, vmem, vmem),
        scratch_shapes=[
            pltpu.SMEM(members.shape, jnp.int32),
            pltpu.VMEM(blk, F32),
            pltpu.VMEM((rb, cb) + blk, BF),
            pltpu.VMEM((level, cs) + blk, BF),
            pltpu.VMEM((n_col, rows, side), BF),
            pltpu.VMEM((n_col, rows, side), BF),
            pltpu.VMEM((nz, rows, side), BF),
            pltpu.VMEM((nz + 1, rows, side), BF),
            pltpu.VMEM((nz + 1, nf * pz, side), BF),
            pltpu.VMEM((level, cs) + blk, BF),
            pltpu.VMEM((level // CORES, cs) + blk, BF),
            pltpu.VMEM((n_row // CORES, kr, cs) + blk, BF),
            pltpu.VMEM((2, side, side // 2), BF),
            pltpu.VMEM((n_row, 2, side, side // 2), BF),
            pltpu.VMEM((max(rs, kr * cs) * side, side), F32),
            pltpu.VMEM((2, side, side // 2), F32),
            dma((5,)), dma((13,)), dma((n_row,)), dma((nz + 1,)), dma((nz, 3)),
            dma((nz, nyp)), dma((nf,)), dma((nz + 1, nyp)), dma((nz + 1, nf)),
            dma((nz + 1, nf)), dma((n_col // CORES,)), dma((n_row // CORES, kr)), dma((n_row, 2)),
        ],
        compiler_params=pltpu.CompilerParams(
            collective_id=0, has_side_effects=True, vmem_limit_bytes=60 * 1024 * 1024
        ),
    )(members, ancestor_inv, lower_panel, upper_panel.reshape(per_col, rows, side), pivot_inv)
    return pl.pallas_call(
        hand_over,
        out_shape=(
            jax.ShapeDtypeStruct((per_col, rs) + blk, BF),
            jax.ShapeDtypeStruct((kr, cs) + blk, BF),
            jax.ShapeDtypeStruct((per_col,) + blk, F32),
        ),
        in_specs=[vmem] * 3,
        out_specs=(hbm,) * 3,
        scratch_shapes=[dma((rs + 2,))],
    )(*(pltpu.with_memory_space_constraint(o, pltpu.VMEM) for o in outs))


def solution(mesh):
    return jax.shard_map(
        body,
        mesh=mesh,
        in_specs=(
            P("row", "col", None, None),
            P("row", "col", None, None),
            P("col", "row", None, None),
            P("col", None, None),
            P(),
        ),
        out_specs=(P("col", "row", None, None), P("row", "col", None, None), P("col", None, None)),
        check_vma=False,
    )
```

```python
import functools

import jax
import jax.numpy as jnp
from jax import lax
from jax.experimental import pallas as pl
from jax.experimental.pallas import tpu as pltpu
from jax.sharding import PartitionSpec as P

NY = 2
CORES = 2
BF = jnp.bfloat16
F32 = jnp.float32


def kernel(
    n_row, n_col, nq, nf, pz, nyp, py,
    mem_in, anc, low, upp, piv_in,
    low_out, upp_out, diag_out,
    mem, piv, a, lbuf, ubuf, pl_buf, yr, zr, zq, pu, pr, ur, ds, dr, acc, dacc,
    loc, sent, l_r, uy_r, uz_r, ry_r, rh_r, rz_r, rf_r, rq_r,
    pr_r, pu_r, d_r,
):
    row = lax.axis_index("row")
    col = lax.axis_index("col")
    nz = n_col // NY
    nx = n_row // CORES
    x, core = row // CORES, row % CORES
    z, y = col // NY, col % NY
    yp = z * NY + (1 - y)
    rb, cb = anc.shape[0], anc.shape[1]
    kr, cs = low.shape[0], low.shape[1]
    side = low.shape[2]
    rows = upp.shape[1]
    rs = rows // side
    ny = rows - nq
    yf = nyp * py
    partner = x * CORES + (1 - core)

    def remote(src, dst, ss, rsem, **where):
        return pltpu.make_async_remote_copy(
            src_ref=src, dst_ref=dst, send_sem=ss, recv_sem=rsem, device_id=where
        )

    ca = pltpu.make_async_copy(anc, a, loc.at[0])
    cl = pltpu.make_async_copy(low, lbuf.at[pl.ds(row * kr, kr)], loc.at[1])
    cu = pltpu.make_async_copy(upp.at[0], ubuf.at[col], loc.at[2])
    cp = pltpu.make_async_copy(piv_in.at[0], piv, loc.at[3])
    cm = pltpu.make_async_copy(mem_in, mem, loc.at[4])

    bar = pltpu.get_barrier_semaphore()
    for dx in range(1, n_row):
        pl.semaphore_signal(bar, inc=1, device_id={"row": (row + dx) % n_row})
    pl.semaphore_signal(bar, inc=1, device_id={"col": yp})

    @pl.when(z > 0)
    def _():
        pl.semaphore_signal(bar, inc=1, device_id={"col": col - NY})

    @pl.when(z < nz - 1)
    def _():
        pl.semaphore_signal(bar, inc=1, device_id={"col": col + NY})

    cu.start()
    cl.start()
    ca.start()
    cm.start()
    cp.start()
    peers = n_row + jnp.where(z > 0, 1, 0) + jnp.where(z < nz - 1, 1, 0)
    pl.semaphore_wait(bar, peers)

    L_S, UA_S, UY_S, RY_S, RH_S, RZ_S, RQ_S, PR_S, PU_S, D_S, UZ_S = range(11)

    def l_own(r2):
        blk = lbuf.at[pl.ds(row * kr, kr)]
        return remote(blk, blk, sent.at[L_S], l_r.at[row], row=r2)

    def l_recv(r2):
        blk = lbuf.at[pl.ds(r2 * kr, kr)]
        return remote(blk, blk, sent.at[L_S], l_r.at[r2], row=partner)

    def uy(k, late, rsem):
        part = pl.ds(0, ny) if late else pl.ds(ny, nq)
        blk = ubuf.at[k, part]
        return remote(blk, blk, sent.at[UY_S if late else UA_S], uy_r.at[rsem], col=yp)

    def uy_own(kind):
        return uy(col, kind == 1, z if kind else nz)

    def uy_got(kind, zs):
        return uy(zs * NY + (1 - y), kind == 1, zs if kind else nz)

    def uy_pass(zs):
        return uy(zs * NY + y, True, zs)

    def uz(zs, kind, up):
        k = zs * NY + (1 - y if kind == 2 else y)
        blk = ubuf.at[k, pl.ds(0, ny) if kind == 0 else pl.ds(ny, nq)]
        to = col + NY if up else col - NY
        return remote(blk, blk, sent.at[UZ_S + kind], uz_r.at[zs if up else zs - 1, kind], col=to)

    half = side // 2
    nh = nyp // 2

    def ypart(h):
        return (
            pl.ds(pl.multiple_of((h % nh) * (2 * py), 16), 2 * py),
            pl.ds(pl.multiple_of((h // nh) * half, half), half),
        )

    def zrows(f, base=yf):
        return pl.ds(pl.multiple_of(base + f * pz, 16), pz)

    def ry(zd, h):
        part = ypart(h)
        return remote(
            pl_buf.at[zd * NY + (1 - y), *part], yr.at[zd, *part], sent.at[RY_S],
            ry_r.at[zd, h], col=yp,
        )

    def rh(f):
        part = zrows(f)
        return remote(pl_buf.at[yp, part], yr.at[z, part], sent.at[RH_S], rh_r.at[f], col=yp)

    def rz(zd, h, up):
        slot = zd + 1 if up else zd
        to = col + NY if up else col - NY
        part = ypart(h)
        return remote(
            pl_buf.at[zd * NY + y, *part], zr.at[slot, *part], sent.at[RZ_S],
            rz_r.at[slot, h], col=to,
        )

    def rf(zd, f, up):
        slot = zd + 1 if up else zd
        to = col + NY if up else col - NY
        part = zrows(f)
        return remote(
            pl_buf.at[zd * NY + y, part], zr.at[slot, part], sent.at[RZ_S],
            rf_r.at[slot, f], col=to,
        )

    def rq(zd, f, up):
        slot = zd + 1 if up else zd
        to = col + NY if up else col - NY
        return remote(
            pl_buf.at[zd * NY + (1 - y), zrows(f)], zq.at[slot, zrows(f, 0)], sent.at[RQ_S],
            rq_r.at[slot, f], col=to,
        )

    def held(k):
        return k // (kr * CORES) * kr + k % kr

    def pr_copy(k):
        slot = held(k)
        return remote(pu.at[k], pr.at[slot], sent.at[PR_S], pr_r.at[slot], row=partner)

    def pu_copy(k):
        return remote(pu.at[k], ur.at[x, k % kr], sent.at[PU_S], pu_r.at[0], row=k // kr)

    def keeps(k):
        return (k // kr) % CORES == core

    def leaves(k):
        return k // (kr * CORES) != x

    def d_copy(r2, c):
        return remote(ds.at[c], dr.at[row, c], sent.at[D_S], d_r.at[row, c], row=r2)

    def d_got(r2, c):
        return remote(ds.at[c], dr.at[r2, c], sent.at[D_S], d_r.at[r2, c], row=r2)

    def d_relay(x2, c):
        r2 = x2 * CORES + core
        blk = dr.at[r2, c]
        return remote(blk, blk, sent.at[D_S], d_r.at[r2, c], row=partner)

    def each_dir(fn):
        @pl.when(z > 0)
        def _():
            fn(False)

        @pl.when(z < nz - 1)
        def _():
            fn(True)

    def row_member(k, i):
        m = mem[k, row * rs + i]
        return m >= 0, jnp.clip(m - row * rb, 0, rb - 1)

    def col_member(k, j):
        m = mem[k, col * cs + j]
        return m >= 0, jnp.clip(m - col * cb, 0, cb - 1)

    planes = nz // nx
    edge = jnp.logical_or(z == 0, z == nz - 1)

    def mine(zs):
        return zs // planes == x

    def last_to(up):
        e = nz - 1 if up else 0
        return jnp.where(mine(e), nz - 2 if up else 1, nz - 1 - e)

    def held_back(zs, up):
        return jnp.logical_and(z == (nz - 2 if up else 1), zs == last_to(up))

    def order(i):
        near_half = jnp.where(i % 2 == 0, nz // 2 + i // 2, i // 2)
        dist = jnp.where(mine(z), near_half, i)
        inner_low = jnp.where(i < nz // 2, nz // 2 + i, nz - 1 - i)
        inner_high = jnp.where(i < nz // 2, nz // 2 - 1 - i, i)
        return jnp.where(
            edge, jnp.where(z == 0, dist, nz - 1 - dist),
            jnp.where(2 * x < nx, inner_low, inner_high),
        )

    zero = jnp.zeros((), BF)

    def block(i):
        return pl.ds(pl.multiple_of(i * side, side), side)

    def lower_part(k):
        cols = [col_member(k, j) for j in range(cs)]
        panels = [jnp.where(cols[j][0], lbuf[k, j], zero) for j in range(cs)]

        def one(i, _):
            ok, ri = row_member(k, i)
            tot = None
            for j in range(cs):
                t = jnp.dot(a[ri, cols[j][1]], panels[j], preferred_element_type=F32)
                tot = t if tot is None else tot + t
            pl_buf[k, block(i)] = jnp.where(ok, tot, 0.0).astype(BF)
            return 0

        lax.fori_loop(0, rs, one, 0)

    def upper_part(k):
        mem_rows = [row_member(k, i) for i in range(rs)]

        def one(j, _):
            ok, cj = col_member(k, j)
            tot = None
            for i in range(rs):
                t = jnp.dot(
                    jnp.where(mem_rows[i][0], ubuf[k, block(i)], zero), a[mem_rows[i][1], cj],
                    preferred_element_type=F32,
                )
                tot = t if tot is None else tot + t
            pu[k, j] = jnp.where(ok, tot, 0.0).astype(BF)
            return 0

        lax.fori_loop(0, cs, one, 0)

        @pl.when(jnp.logical_not(keeps(k)))
        def _():
            pr_copy(k).start()

    def finish(k):
        @pl.when(jnp.logical_and(keeps(k), leaves(k)))
        def _():
            pr_copy(k).wait_recv()
            for j in range(cs):
                pu[k, j] = (pu[k, j].astype(F32) + pr[held(k), j].astype(F32)).astype(BF)
            pu_copy(k).start()

    def lower_group(r2):
        def one(p, _):
            k = r2 * kr + (p + 1 - y) % NY
            lower_part(k)

            @pl.when(k % NY != y)
            def _():
                for h in range(nyp):
                    ry(k // NY, h).start()

            return 0

        lax.fori_loop(0, kr, one, 0)

    def both_groups(x2):
        def one(q, _):
            lower_group(x2 * CORES + jnp.where(2 * x2 >= nx, CORES - 1 - q, q))
            return 0

        lax.fori_loop(0, CORES, one, 0)

    cu.wait()
    uy_own(0).start()
    each_dir(lambda up: uz(z, 0, up).start())
    each_dir(lambda up: uz(z, 1, up).start())
    cl.wait()
    l_own(partner).start()
    for dx in range(1, nx):
        l_own(((x + dx) % nx) * CORES + core).start()
    cm.wait()
    ca.wait()
    l_recv(partner).wait_recv()
    both_groups(x)

    uy_got(0, z).wait_recv()

    def share(zs, up):
        @pl.when(jnp.logical_not(held_back(zs, up)))
        def _():
            uz(zs, 2, up).start()

    each_dir(lambda up: share(z, up))
    upper_part(col)

    def others(fn):
        for dx in range(1, nx):
            fn((x + dx) % nx)

    def add_to(k, part, terms):
        tot = pl_buf[k, *part].astype(F32)
        for t in terms:
            tot = tot + t.astype(F32)
        pl_buf[k, *part] = tot.astype(BF)

    def each_way(zd, go):
        @pl.when(zd > z)
        def _():
            go(True)

        @pl.when(zd < z)
        def _():
            go(False)

    def hop_f(zd, f, own):
        k = zd * NY + (y if own else 1 - y)
        part = zrows(f)

        def go(up):
            slot = zd + 1 if up else zd
            step = (rf if own else rq)(zd, f, up)

            @pl.when((z > 0) if up else (z < nz - 1))
            def _():
                step.wait_recv()
                add_to(k, (part,), [zr[slot, part] if own else zq[slot, zrows(f, 0)]])

            step.start()

        each_way(zd, go)

    def hop_y(zd, h):
        k = zd * NY + y
        part = ypart(h)

        def go(up):
            slot = zd + 1 if up else zd
            step = rz(zd, h, up)
            ry(zd, h).wait_recv()

            @pl.when((z > 0) if up else (z < nz - 1))
            def _():
                step.wait_recv()
                add_to(k, part, [yr[zd, *part], zr[slot, *part]])

            @pl.when((z == 0) if up else (z == nz - 1))
            def _():
                add_to(k, part, [yr[zd, *part]])

            step.start()

        each_way(zd, go)

    def firsts(zds, own):
        def one(f, _):
            for zd, ok in zds:
                @pl.when(ok)
                def _():
                    hop_f(zd, f, own)

            return 0

        lax.fori_loop(0, nf, one, 0)

    def ends(j):
        return [(jnp.where(z == 0, nz - 1 - j, j), j < nz - 1)]

    def opening(early):
        def one(j, _):
            zd = ends(j)[0][0]
            firsts([(zd, mine(zd) if early else jnp.logical_not(mine(zd)))], False)
            return 0

        lax.fori_loop(0, nz - 1, one, 0)

    def relay(x2):
        l_recv(x2 * CORES + core).wait_recv()
        l_recv(x2 * CORES + core).start()

    def by_side(d, fn):
        @pl.when(z - d >= 0)
        def _():
            fn(z - d, True)

        @pl.when(z + d <= nz - 1)
        def _():
            fn(z + d, False)

    def take(kind):
        def one(zs, up):
            uz(zs, kind, up).wait_recv()

            @pl.when((z < nz - 1) if up else (z > 0))
            def _():
                if kind == 2:
                    share(zs, up)
                else:
                    uz(zs, kind, up).start()

        return one

    by_side(1, take(0))

    @pl.when(edge)
    def _():
        opening(True)

    others(relay)
    by_side(1, take(1))

    def late(x2):
        l_recv(x2 * CORES + 1 - core).wait_recv()
        both_groups(x2)

    others(late)

    @pl.when(edge)
    def _():
        opening(False)

    @pl.when(jnp.logical_not(edge))
    def _():
        by_side(1, take(2))

    def hand_on(zs):
        @pl.when(zs == z)
        def _():
            uy_own(1).start()

        @pl.when(zs != z)
        def _():
            uy_pass(zs).start()

    def sides(d, fn):
        def one(s, _):
            zs = z + (2 * s - 1) * d

            @pl.when(jnp.logical_and(zs >= 0, zs < nz))
            def _():
                fn(zs)

            return 0

        lax.fori_loop(0, 2, one, 0)

    def near(d):
        sides(d, lambda zs: upper_part(zs * NY + y))

    def near_done(d):
        sides(d, lambda zs: finish(zs * NY + y))

    def across(i):
        zs = order(i)

        @pl.when(jnp.logical_and(edge, zs > z))
        def _():
            uz(zs, 2, False).wait_recv()

        @pl.when(jnp.logical_and(edge, zs < z))
        def _():
            uz(zs, 2, True).wait_recv()

        uy_got(1, zs).wait_recv()
        upper_part(zs * NY + (1 - y))

    def across_done(i):
        finish(order(i) * NY + (1 - y))

    def home():
        def one(f, _):
            each_dir(lambda up: rq(z, f, not up).wait_recv())

            @pl.when(z > 0)
            def _():
                add_to(yp, (zrows(f),), [zq[z + 1, zrows(f, 0)]])

            @pl.when(z < nz - 1)
            def _():
                add_to(yp, (zrows(f),), [zq[z, zrows(f, 0)]])

            rh(f).start()
            return 0

        lax.fori_loop(0, nf, one, 0)

    def seconds(zds, hook=None, close=None):
        def piece(h, _):
            if hook is not None:
                hook(h)
            for zd, ok in zds:
                @pl.when(ok)
                def _():
                    hop_y(zd, h)

                if close is not None and zd is zds[0][0]:
                    @pl.when(h == nyp - 1)
                    def _():
                        close()

            return 0

        lax.fori_loop(0, nyp, piece, 0)

    near(1)
    finish(col)

    @pl.when(edge)
    def _():
        firsts(ends(0), True)
        seconds(ends(0))
        firsts(ends(1), True)

        def on(dist):
            hand_on(jnp.where(z == 0, dist, nz - 1 - dist))

        def one(d, _):
            by_side(d, take(0))

            @pl.when(jnp.logical_and(mine(z), d >= nz // 2))
            def _():
                on(d)

                @pl.when(d < nz - 1)
                def _():
                    on(d - nz // 2)

            @pl.when(jnp.logical_not(mine(z)))
            def _():
                @pl.when(d == 2)
                def _():
                    on(0)
                    on(1)

                @pl.when(d < nz - 1)
                def _():
                    on(d)

            by_side(d, take(1))
            near(d)
            near_done(d - 1)
            seconds(ends(d - 1))
            firsts(ends(d), True)
            return 0

        lax.fori_loop(2, nz, one, 0)
        across(0)
        near_done(nz - 1)
        home()
        hand_on(order(nz - 1))
        across(1)
        across_done(0)

    @pl.when(jnp.logical_not(edge))
    def _():
        low_half = 2 * z < nz
        short = jnp.where(low_half, z, nz - 1 - z)
        gap = nz - 1 - 2 * short
        spot = nyp - 2

        def both(s):
            s2 = s - gap
            return [
                (
                    jnp.where(low_half, s2, nz - 1 - s2),
                    jnp.logical_and(s2 >= 0, s2 < short),
                ),
                (jnp.where(low_half, nz - 1 - s, s), s >= 0),
            ]

        def others_long(s, _):
            firsts(both(s)[1:], False)
            return 0

        def others_short(s, _):
            firsts(both(s)[:1], False)
            return 0

        def one(d, _):
            by_side(d, take(0))

            @pl.when(d == nz - 2)
            def _():
                for i in range(nz - 1):
                    hand_on(order(i))

            by_side(d, take(1))

            @pl.when(d == nz - 2)
            def _():
                lax.fori_loop(0, nz - 1 - short, others_long, 0)

            by_side(d, take(2))
            near(d)
            near_done(d - 1)
            return 0

        lax.fori_loop(2, nz - 1, one, 0)
        def pair(s, _):
            s2 = s - gap

            def hook(h):
                now = s == nz - 2 - short

                @pl.when(jnp.logical_and(now, h - spot == 0))
                def _():
                    near_done(nz - 2)
                    across(0)

                @pl.when(jnp.logical_and(now, h - spot == 1))
                def _():
                    across(1)

            def close():
                @pl.when(s2 == short - 1)
                def _():
                    @pl.when(z == 1)
                    def _():
                        uz(last_to(False), 2, False).start()

                    @pl.when(z == nz - 2)
                    def _():
                        uz(last_to(True), 2, True).start()

            firsts(both(s), True)

            @pl.when(s == 0)
            def _():
                lax.fori_loop(0, nz - 1 - short, others_short, 0)

            seconds(both(s), hook, close)

            @pl.when(s == 0)
            def _():
                home()
                hand_on(order(nz - 1))

            return 0

        lax.fori_loop(0, nz - 1 - short, pair, 0)
        across_done(0)

    across_done(1)

    def rest(i, _):
        across(i)

        @pl.when(i > 2)
        def _():
            across_done(i - 1)

        return 0

    lax.fori_loop(2, nz - 1, rest, 0)

    def final(part, got, step):
        got.wait_recv()
        acc[*part] = pl_buf[col, *part].astype(F32) + yr[z, *part].astype(F32)

        @pl.when(z > 0)
        def _():
            step(True).wait_recv()
            acc[*part] = acc[*part] + zr[z + 1, *part].astype(F32)

        @pl.when(z < nz - 1)
        def _():
            step(False).wait_recv()
            acc[*part] = acc[*part] + zr[z, *part].astype(F32)

        low_out[0, *part] = (-acc[*part]).astype(BF)

    def final_f(f, _):
        final((zrows(f),), rh(f), lambda up: rf(z, f, up))
        return 0

    def final_y(h, _):
        final(ypart(h), ry(z, h), lambda up: rz(z, h, up))
        return 0

    lax.fori_loop(0, nf, final_f, 0)

    def side_sum(c, _):
        lax.fori_loop(c * nh, (c + 1) * nh, final_y, 0)
        cols = pl.ds(pl.multiple_of(c * half, half), half)
        tot = None
        for i in range(rs):
            t = jnp.dot(
                jnp.where(row_member(col, i)[0], ubuf[col, block(i)], zero),
                low_out[0, block(i), cols],
                preferred_element_type=F32,
            )
            tot = t if tot is None else tot + t
        dacc[c] = tot
        ds[c] = tot.astype(BF)
        others(lambda x2: d_copy(x2 * CORES + core, c).start())
        d_copy(partner, c).start()
        return 0

    lax.fori_loop(0, 2, side_sum, 0)

    across_done(nz - 2)

    def d_pass(x2):
        for c in range(2):
            d_got(x2 * CORES + core, c).wait_recv()
            d_relay(x2, c).start()

    @pl.when(edge)
    def _():
        others(d_pass)

    across(nz - 1)
    across_done(nz - 1)

    @pl.when(jnp.logical_not(edge))
    def _():
        others(d_pass)

    def piece(p, j):
        return block(p * cs + j)

    for p in range(kr):
        pr_copy(row * kr + p).wait_recv()
        for j in range(cs):
            acc[piece(p, j)] = (
                pu[row * kr + p, j].astype(F32) + pr[held(row * kr + p), j].astype(F32)
            )

    def pu_add(x2):
        for p in range(kr):
            for j in range(cs):
                acc[piece(p, j)] = acc[piece(p, j)] + ur[x2, p, j].astype(F32)

    some = ur.at[pl.ds(0, nx - 1)]
    pltpu.make_async_copy(some, some, pu_r.at[0]).wait()
    others(pu_add)
    for p in range(kr):
        for j in range(cs):
            upp_out[p, j] = (-acc[piece(p, j)]).astype(BF)

    def all_sent(ref, which):
        pltpu.make_async_copy(ref, ref, sent.at[which]).wait()

    for kind in range(3):
        n = nq if kind else ny

        @pl.when(edge)
        def _():
            all_sent(ubuf.at[pl.ds(0, 1), pl.ds(0, n)], UZ_S + kind)

        @pl.when(jnp.logical_not(edge))
        def _():
            all_sent(ubuf.at[pl.ds(0, nz + 1), pl.ds(0, n)], UZ_S + kind)

    all_sent(lbuf.at[pl.ds(0, kr * (2 * nx - 1))], L_S)
    all_sent(ubuf.at[pl.ds(0, 1), pl.ds(0, nq)], UA_S)
    all_sent(ubuf.at[pl.ds(0, nz), pl.ds(0, ny)], UY_S)
    all_sent(pl_buf.at[pl.ds(0, nz), pl.ds(0, yf)], RY_S)
    all_sent(pl_buf.at[pl.ds(0, 1), pl.ds(0, nf * pz)], RH_S)
    all_sent(pl_buf.at[pl.ds(0, nz - 1)], RZ_S)
    all_sent(pl_buf.at[pl.ds(0, nz - 1), pl.ds(0, nf * pz)], RQ_S)
    all_sent(pu.at[pl.ds(0, n_col // CORES)], PR_S)
    all_sent(pu.at[pl.ds(0, kr * (nx - 1))], PU_S)

    cp.wait()

    def d_sum(c, _):
        def d_add(r2):
            dacc[c] = dacc[c] + dr[r2, c].astype(F32)

        d_got(partner, c).wait_recv()
        d_add(partner)

        def d_add_chip(x2):
            d_add(x2 * CORES + core)
            d_got(x2 * CORES + 1 - core, c).wait_recv()
            d_add(x2 * CORES + 1 - core)

        others(d_add_chip)
        cols = pl.ds(pl.multiple_of(c * half, half), half)
        diag_out[0, :, cols] = piv[:, cols] - dacc[c]
        return 0

    lax.fori_loop(0, 2, d_sum, 0)
    all_sent(dr.at[pl.ds(0, 2 * nx - 1)], D_S)


def hand_over(low, upp, diag, low_to, upp_to, diag_to, sems):
    side = diag.shape[1]
    pairs = [(upp, upp_to), (diag, diag_to)]
    for h in range(low_to.shape[1]):
        pairs.append((low.at[0, pl.ds(h * side, side)], low_to.at[0, h]))
    copies = [pltpu.make_async_copy(a, b, sems.at[i]) for i, (a, b) in enumerate(pairs)]
    for c in copies:
        c.start()
    for c in copies:
        c.wait()


def body(ancestor_inv, lower_panel, upper_panel, pivot_inv, members):
    n_col = lax.axis_size("col")
    n_row = lax.axis_size("row")
    side = ancestor_inv.shape[2]
    rb, cb = ancestor_inv.shape[:2]
    kr, cs = lower_panel.shape[:2]
    per_col, rs = upper_panel.shape[:2]
    level = members.shape[0]
    nz = n_col // NY
    assert per_col == 1 and level == n_col and kr == NY and nz == n_row
    rows = rs * side
    nf, nyp = 1, 2
    pz = rows * 3 // 8
    py = (rows - nf * pz) // nyp
    nq = rows * 13 // 32
    assert nf * pz + nyp * py == rows and pz % 16 == 0 and py % 16 == 0 and nq % 16 == 0
    blk = (side, side)
    dma = pltpu.SemaphoreType.DMA
    vmem = pl.BlockSpec(memory_space=pltpu.VMEM)
    hbm = pl.BlockSpec(memory_space=pltpu.HBM)
    outs = pl.pallas_call(
        functools.partial(kernel, n_row, n_col, nq, nf, pz, nyp, py),
        out_shape=(
            pltpu.VMEM((per_col, rows, side), BF),
            pltpu.VMEM((kr, cs) + blk, BF),
            pltpu.VMEM((per_col,) + blk, F32),
        ),
        in_specs=[hbm] * 5,
        out_specs=(vmem, vmem, vmem),
        scratch_shapes=[
            pltpu.SMEM(members.shape, jnp.int32),
            pltpu.VMEM(blk, F32),
            pltpu.VMEM((rb, cb) + blk, BF),
            pltpu.VMEM((level, cs) + blk, BF),
            pltpu.VMEM((n_col, rows, side), BF),
            pltpu.VMEM((n_col, rows, side), BF),
            pltpu.VMEM((nz, rows, side), BF),
            pltpu.VMEM((nz + 1, rows, side), BF),
            pltpu.VMEM((nz + 1, nf * pz, side), BF),
            pltpu.VMEM((level, cs) + blk, BF),
            pltpu.VMEM((level // CORES, cs) + blk, BF),
            pltpu.VMEM((n_row // CORES, kr, cs) + blk, BF),
            pltpu.VMEM((2, side, side // 2), BF),
            pltpu.VMEM((n_row, 2, side, side // 2), BF),
            pltpu.VMEM((max(rs, kr * cs) * side, side), F32),
            pltpu.VMEM((2, side, side // 2), F32),
            dma((5,)), dma((13,)), dma((n_row,)), dma((nz + 1,)), dma((nz - 1, 3)),
            dma((nz, nyp)), dma((nf,)), dma((nz + 1, nyp)), dma((nz + 1, nf)),
            dma((nz + 1, nf)), dma((n_col // CORES,)), dma((1,)), dma((n_row, 2)),
        ],
        compiler_params=pltpu.CompilerParams(
            collective_id=0, has_side_effects=True, vmem_limit_bytes=60 * 1024 * 1024
        ),
    )(members, ancestor_inv, lower_panel, upper_panel.reshape(per_col, rows, side), pivot_inv)
    return pl.pallas_call(
        hand_over,
        out_shape=(
            jax.ShapeDtypeStruct((per_col, rs) + blk, BF),
            jax.ShapeDtypeStruct((kr, cs) + blk, BF),
            jax.ShapeDtypeStruct((per_col,) + blk, F32),
        ),
        in_specs=[vmem] * 3,
        out_specs=(hbm,) * 3,
        scratch_shapes=[dma((rs + 2,))],
    )(*(pltpu.with_memory_space_constraint(o, pltpu.VMEM) for o in outs))


def solution(mesh):
    return jax.shard_map(
        body,
        mesh=mesh,
        in_specs=(
            P("row", "col", None, None),
            P("row", "col", None, None),
            P("col", "row", None, None),
            P("col", None, None),
            P(),
        ),
        out_specs=(P("col", "row", None, None), P("row", "col", None, None), P("col", None, None)),
        check_vma=False,
    )
```
